16 devices in a mesh: data: 2 (over z), col: 2 (over y), row: 4 (over x, core).
Axes of the slice: x: 2, y: 2, z: 2, core: 2. Of those that a mesh axis runs over, the one named last changes fastest.
Arguments:
- x_in: bfloat16 [2048, 2048], P(None, 'row')
- h_act: bfloat16 [2048, 5632], P(None, 'row')
- d_gate: bfloat16 [2048, 5632], P(None, 'col')
- d_up: bfloat16 [2048, 5632], P(None, 'col')
- d_out: bfloat16 [2048, 2048], P(None, 'col')
- w_gate: float32 [2048, 5632], P('row', 'col')
- w_up: float32 [2048, 5632], P('row', 'col')
- w_down: float32 [5632, 2048], P('row', 'col')
- r_gate: float32 [2048], P('row')
- c_gate: float32 [5632], P('col')
- r_up: float32 [2048], P('row')
- c_up: float32 [5632], P('col')
- r_down: float32 [5632], P('row')
- c_down: float32 [2048], P('col')
- beta_two: float32 [], replicated
- rel_step: float32 [], replicated
- clip_thr: float32 [], replicated
Outputs:
- output 1: float32 [2048, 5632], P('row', 'col')
- output 2: float32 [2048, 5632], P('row', 'col')
- output 3: float32 [5632, 2048], P('row', 'col')
- output 4: float32 [2048], P('row')
- output 5: float32 [5632], P('col')
- output 6: float32 [2048], P('row')
- output 7: float32 [5632], P('col')
- output 8: float32 [5632], P('row')
- output 9: float32 [2048], P('col')
All inputs are finite; a program needn't handle non-finite values.
Results may differ from the reference program's by a relative error of at most 0.001.
Values are sent between devices in bfloat16 or wider.
A program may use at most 1 GiB of HBM per device.

```python
import jax
import jax.numpy as jnp

TOKENS = 2048
D = 2048
FF = 5632

EPS_SQ = 1e-30
EPS_SCALE = 1e-3
DOWN_STAT_SCALE = 60.0


def weight_grad(act_in, cot_out):
    return jnp.dot(act_in.T, cot_out, preferred_element_type=jnp.float32)


def adafactor_step(w_mat, g_mat, r_old, c_old, beta_two, rel_step, clip_thr):
    q_mat = g_mat * g_mat + EPS_SQ
    r_new = beta_two * r_old + (1.0 - beta_two) * jnp.mean(q_mat, axis=1)
    c_new = beta_two * c_old + (1.0 - beta_two) * jnp.mean(q_mat, axis=0)
    v_mat = r_new[:, None] * c_new[None, :] / jnp.mean(r_new)
    u_mat = g_mat / jnp.sqrt(v_mat)
    u_rms = jnp.sqrt(jnp.mean(u_mat * u_mat))
    u_hat = u_mat / jnp.maximum(1.0, u_rms / clip_thr)
    w_rms = jnp.sqrt(jnp.mean(w_mat * w_mat))
    step_size = rel_step * jnp.maximum(EPS_SCALE, w_rms)
    return w_mat - step_size * u_hat, r_new, c_new


def old_stats(g_mat, key_row, key_col, stat_scale):
    q_mat = g_mat * g_mat
    row_fac = jnp.exp(jax.random.uniform(key_row, (g_mat.shape[0],), jnp.float32, -1.2, 1.2))
    col_fac = jnp.exp(jax.random.uniform(key_col, (g_mat.shape[1],), jnp.float32, -1.2, 1.2))
    return stat_scale * jnp.mean(q_mat, axis=1) * row_fac, stat_scale * jnp.mean(q_mat, axis=0) * col_fac


def setup_inputs(seed: int = 0) -> dict:
    key_list = jax.random.split(jax.random.key(seed), 17)
    x_in = jax.random.normal(key_list[0], (TOKENS, D), jnp.float32).astype(jnp.bfloat16)
    h_act = jax.random.normal(key_list[1], (TOKENS, FF), jnp.float32).astype(jnp.bfloat16)
    d_gate = jax.random.normal(key_list[2], (TOKENS, FF), jnp.float32).astype(jnp.bfloat16)
    d_up = jax.random.normal(key_list[3], (TOKENS, FF), jnp.float32).astype(jnp.bfloat16)
    d_out = jax.random.normal(key_list[4], (TOKENS, D), jnp.float32).astype(jnp.bfloat16)
    w_gate = jax.random.normal(key_list[5], (D, FF), jnp.float32) * D ** -0.5
    w_up = jax.random.normal(key_list[6], (D, FF), jnp.float32) * D ** -0.5
    w_down = jax.random.normal(key_list[7], (FF, D), jnp.float32) * FF ** -0.5
    r_gate, c_gate = old_stats(weight_grad(x_in, d_gate), key_list[8], key_list[9], 1.0)
    r_up, c_up = old_stats(weight_grad(x_in, d_up), key_list[10], key_list[11], 1.0)
    r_down, c_down = old_stats(weight_grad(h_act, d_out), key_list[12], key_list[13], DOWN_STAT_SCALE)
    beta_two = jax.random.uniform(key_list[14], (), jnp.float32, 0.5, 0.9)
    rel_step = jax.random.uniform(key_list[15], (), jnp.float32, 0.2, 0.6)
    clip_thr = jax.random.uniform(key_list[16], (), jnp.float32, 0.4, 0.6)
    return dict(x_in=x_in, h_act=h_act, d_gate=d_gate, d_up=d_up, d_out=d_out, w_gate=w_gate, w_up=w_up, w_down=w_down, r_gate=r_gate, c_gate=c_gate, r_up=r_up, c_up=c_up, r_down=r_down, c_down=c_down, beta_two=beta_two, rel_step=rel_step, clip_thr=clip_thr)


def reference(x_in, h_act, d_gate, d_up, d_out, w_gate, w_up, w_down, r_gate, c_gate, r_up, c_up, r_down, c_down, beta_two, rel_step, clip_thr):
    gate_w, gate_r, gate_c = adafactor_step(w_gate, weight_grad(x_in, d_gate), r_gate, c_gate, beta_two, rel_step, clip_thr)
    up_w, up_r, up_c = adafactor_step(w_up, weight_grad(x_in, d_up), r_up, c_up, beta_two, rel_step, clip_thr)
    down_w, down_r, down_c = adafactor_step(w_down, weight_grad(h_act, d_out), r_down, c_down, beta_two, rel_step, clip_thr)
    return (gate_w, up_w, down_w, gate_r, gate_c, up_r, up_c, down_r, down_c)
```

```python
import jax
import jax.numpy as jnp
from jax import lax
from jax.experimental import pallas as pl
from jax.experimental.pallas import tpu as pltpu
from jax.sharding import PartitionSpec as P

EPS_SQ = 1e-30
EPS_SCALE = 1e-3
LANES = 128
K = 2048
ROWS, COLS = 4, 2
F32 = jnp.float32
BF16 = jnp.bfloat16
MESH = pl.DeviceIdType.MESH

SHAPES = ((512, 2816), (512, 2816), (1408, 1024))
TOTALS = tuple((m * ROWS, n * COLS) for m, n in SHAPES)
BLOCKS = (
    (0, 0, 1024), (0, 1024, 2048), (0, 2048, 2816),
    (1, 0, 1024), (1, 1024, 2048), (1, 2048, 2816),
    (2, 0, 512), (2, 512, 1024),
)
SLOTS = 3
SLOT_WIDTH = 1024
HCHUNK = 256
CHUNK = 64


def interleave(dots, units):
    done = 0
    for i, dot in enumerate(dots):
        dot()
        upto = len(units) * (i + 1) // len(dots)
        for unit in units[done:upto]:
            unit()
        done = upto
    for unit in units[done:]:
        unit()


def fold(x):
    return jnp.sum(x.reshape(x.shape[0] // 8, 8, x.shape[1]), axis=0)


def stats_kernel(
    x_hbm, h_hbm, dg_hbm, du_hbm, do_hbm, wg_hbm, wu_hbm, wd_hbm,
    rg, cg, ru, cu, rd, cd, beta, rel, clip,
    hg, hu, hd, wg, wu, wd, rg_new, cg_new, ru_new, cu_new, rd_new, cd_new, kap,
    ring, xs, xt, hs, ht, rowacc, abc_g, abc_u, abc_d, cacc_g, cacc_u, cacc_d,
    bv_g, bv_u, bv_d, rbuf_g, rbuf_u, rbuf_d, cbuf_g, cbuf_u, cbuf_d, sbuf, sacc, wacc,
    ring_sem, x_sem, h_sem, w_sem, r_send, r_recv, c_send, c_recv, s_send, s_recv,
):
    d_hbm = (dg_hbm, du_hbm, do_hbm)
    w_hbm = (wg_hbm, wu_hbm, wd_hbm)
    G = (hg, hu, hd)
    W = (wg, wu, wd)
    r_old, c_old = (rg, ru, rd), (cg, cu, cd)
    r_new, c_new = (rg_new, ru_new, rd_new), (cg_new, cu_new, cd_new)
    abc, cacc, bv = (abc_g, abc_u, abc_d), (cacc_g, cacc_u, cacc_d), (bv_g, bv_u, bv_d)
    rbuf, cbuf = (rbuf_g, rbuf_u, rbuf_d), (cbuf_g, cbuf_u, cbuf_d)

    me_d, me_c, me_r = lax.axis_index("data"), lax.axis_index("col"), lax.axis_index("row")
    me = me_c * ROWS + me_r

    def peer(dc, dr):
        return (me_d, lax.rem(me_c + dc, COLS), lax.rem(me_r + dr, ROWS))

    others = [(dc, dr) for dc in range(COLS) for dr in range(ROWS) if (dc, dr) != (0, 0)]

    def d_copy(j):
        mat, n0, n1 = BLOCKS[j]
        slot = j % SLOTS
        return pltpu.make_async_copy(
            d_hbm[mat].at[:, n0:n1], ring.at[slot, :, : n1 - n0], ring_sem.at[slot])

    XC = 4
    XK = K // XC

    def x_copy(c):
        return pltpu.make_async_copy(x_hbm.at[c * XK:(c + 1) * XK, :], xs.at[c * XK:(c + 1) * XK, :], x_sem.at[c])

    def d0_copy(c):
        n1 = BLOCKS[0][2]
        return pltpu.make_async_copy(
            dg_hbm.at[c * XK:(c + 1) * XK, 0:n1], ring.at[0, c * XK:(c + 1) * XK, 0:n1], x_sem.at[XC + c])

    HS = 4

    def h_copy(c):
        return pltpu.make_async_copy(h_hbm.at[c * HCHUNK:(c + 1) * HCHUNK, :], hs.at[c % HS], h_sem.at[c % HS])

    def w_copy(mat):
        return pltpu.make_async_copy(w_hbm[mat], W[mat], w_sem.at[mat])

    def row_copy(mat):
        return pltpu.make_async_remote_copy(
            src_ref=rbuf[mat].at[me_c], dst_ref=rbuf[mat].at[me_c],
            send_sem=r_send.at[mat], recv_sem=r_recv.at[mat],
            device_id=peer(1, 0), device_id_type=MESH)

    def col_copy(mat, d):
        return pltpu.make_async_remote_copy(
            src_ref=cbuf[mat].at[me_r], dst_ref=cbuf[mat].at[me_r],
            send_sem=c_send.at[mat, d - 1], recv_sem=c_recv.at[mat, d - 1],
            device_id=peer(0, d), device_id_type=MESH)

    def scal_copy(mat, i):
        return pltpu.make_async_remote_copy(
            src_ref=sbuf.at[mat, me], dst_ref=sbuf.at[mat, me],
            send_sem=s_send.at[mat, i], recv_sem=s_recv.at[mat, i],
            device_id=peer(*others[i]), device_id_type=MESH)

    def stats_units(j):
        mat, n0, n1 = BLOCKS[j]
        g_ref = G[mat]
        first = n0 == 0
        units = []
        for r in range(0, SHAPES[mat][0], CHUNK):
            def unit(r=r):
                part = None
                for t in range(n0 // LANES, n1 // LANES):
                    g = g_ref[r:r + CHUNK, t * LANES:(t + 1) * LANES]
                    q = g * g
                    part = q if part is None else part + q
                    col = fold(q)
                    cols = pl.ds(t * LANES, LANES)
                    cacc[mat][:, cols] = col if r == 0 else cacc[mat][:, cols] + col
                rows = pl.ds(r, CHUNK)
                rowacc[rows, :] = part if first else rowacc[rows, :] + part
            units.append(unit)
        return units

    def w2_units(mat):
        units = []
        m, n = SHAPES[mat]
        for r in range(0, m, CHUNK):
            def unit(r=r):
                acc = None
                for t in range(n // LANES):
                    w = W[mat][r:r + CHUNK, t * LANES:(t + 1) * LANES]
                    f = fold(w * w)
                    acc = f if acc is None else acc + f
                wacc[mat] = acc if r == 0 else wacc[mat] + acc
            units.append(unit)
        return units

    def scale_units(mat):
        units = []
        m, n = SHAPES[mat]
        for r in range(0, m, CHUNK):
            def unit(r=r):
                acc = None
                a = abc[mat][r:r + CHUNK, :]
                for t in range(n // LANES):
                    cols = slice(t * LANES, (t + 1) * LANES)
                    h = G[mat][r:r + CHUNK, cols] * a * bv[mat][t:t + 1, :]
                    G[mat][r:r + CHUNK, cols] = h
                    f = fold(h * h)
                    acc = f if acc is None else acc + f
                sacc[mat] = acc if r == 0 else sacc[mat] + acc
            units.append(unit)
        return units

    def transpose_units(c0, c1):
        units = []
        for c in range(c0, c1):
            for i in range(0, SHAPES[2][0], LANES):
                def unit(c=c, i=i):
                    ht[i:i + LANES, c * HCHUNK:(c + 1) * HCHUNK] = hs[c % HS, :, i:i + LANES].T
                units.append(unit)
        return units

    def send_sums(mat):
        m, n = SHAPES[mat]
        for i in range(m // LANES):
            block = rowacc[i * LANES:(i + 1) * LANES, :].T
            rbuf[mat][me_c, i:i + 1, :] = jnp.sum(block, axis=0, keepdims=True)
        for t in range(n // LANES):
            cbuf[mat][me_r, t:t + 1, :] = jnp.sum(
                cacc[mat][:, t * LANES:(t + 1) * LANES], axis=0, keepdims=True)
        row_copy(mat).start()
        for d in (1, 2, 3):
            col_copy(mat, d).start()

    def finish_sums(mat):
        m, n = SHAPES[mat]
        mt, nt = TOTALS[mat]
        row_copy(mat).wait_recv()
        for d in (1, 2, 3):
            col_copy(mat, d).wait_recv()
        b2 = beta[0]
        rows = rbuf[mat][0] + rbuf[mat][1]
        cols = (cbuf[mat][0] + cbuf[mat][1]) + (cbuf[mat][2] + cbuf[mat][3])
        rn = b2 * r_old[mat][...] + (1.0 - b2) * (rows * (1.0 / nt) + EPS_SQ)
        cn = b2 * c_old[mat][...] + (1.0 - b2) * (cols * (1.0 / mt) + EPS_SQ)
        r_new[mat][...] = rn
        c_new[mat][...] = cn
        a = lax.rsqrt(rn)
        bv[mat][...] = lax.rsqrt(cn)
        for i in range(m // LANES):
            abc[mat][i * LANES:(i + 1) * LANES, :] = jnp.broadcast_to(a[i:i + 1, :], (LANES, LANES)).T

    def send_scalars(mat):
        s = jnp.sum(sacc[mat], axis=0, keepdims=True)
        w = jnp.sum(wacc[mat], axis=0, keepdims=True)
        r = jnp.sum(r_new[mat][...], axis=0, keepdims=True)
        sbuf[mat, me] = jnp.concatenate([s, w, r, jnp.zeros((5, LANES), F32)], axis=0)
        for i in range(len(others)):
            scal_copy(mat, i).start()

    def finish_scalars(mat):
        mt, nt = TOTALS[mat]
        for i in range(len(others)):
            scal_copy(mat, i).wait_recv()
        tot = sbuf[mat, 0]
        for i in range(1, ROWS * COLS):
            tot = tot + sbuf[mat, i]
        tot = jnp.sum(tot, axis=1, keepdims=True)
        s, w, r = tot[0:1, :], tot[1:2, :], tot[2:3, :]
        r_mean = r * (1.0 / (COLS * mt))
        u_rms = jnp.sqrt(s * (1.0 / (mt * nt)) * r_mean)
        w_rms = jnp.sqrt(w * (1.0 / (mt * nt)))
        step = rel[0] * jnp.maximum(EPS_SCALE, w_rms)
        k = step * jnp.sqrt(r_mean) / jnp.maximum(1.0, u_rms / clip[0])
        kap[mat] = jnp.broadcast_to(k, (8, LANES))

    def dots_of(j):
        mat, n0, n1 = BLOCKS[j]
        slot = j % SLOTS
        lhs = ht if mat == 2 else xt
        m = SHAPES[mat][0]
        out = []

        def dot(r0, r1, c0, c1):
            def run():
                G[mat][r0:r1, n0 + c0:n0 + c1] = jnp.dot(
                    lhs[r0:r1, :], ring[slot, :, c0:c1], preferred_element_type=F32)
            return run

        mb = 352 if mat == 2 else 512
        w = n1 - n0
        for c in range(0, w, 512):
            if c + 512 <= w:
                out += [dot(r, r + mb, c, c + 512) for r in range(0, m, mb)]
            else:
                out += [dot(0, 256, c, w), dot(256, 512, c, w)]
        return out

    for c in range(XC):
        x_copy(c).start()
        d0_copy(c).start()
    d_copy(1).start()
    d_copy(2).start()

    barrier = pltpu.get_barrier_semaphore()
    for dc, dr in others:
        pl.semaphore_signal(barrier, inc=1, device_id=peer(dc, dr), device_id_type=MESH)

    for c in range(XC):
        x_copy(c).wait()
        d0_copy(c).wait()
        ks = slice(c * XK, (c + 1) * XK)
        for i in range(0, 512, LANES):
            xt[i:i + LANES, ks] = xs[ks, i:i + LANES].T
        for n in range(0, BLOCKS[0][2], 512):
            part = jnp.dot(xt[:, ks], ring[0, ks, n:n + 512], preferred_element_type=F32)
            hg[:, n:n + 512] = part if c == 0 else hg[:, n:n + 512] + part
    d_copy(3).start()
    for c in range(HS):
        h_copy(c).start()

    d_copy(1).wait()
    interleave(dots_of(1), stats_units(0))
    d_copy(4).start()
    w_copy(0).start()

    d_copy(2).wait()
    for c in (0, 1):
        h_copy(c).wait()
    interleave(dots_of(2), stats_units(1) + transpose_units(0, 2))
    d_copy(5).start()
    for c in (4, 5):
        h_copy(c).start()
    pl.semaphore_wait(barrier, len(others))

    d_copy(3).wait()
    for c in (2, 3):
        h_copy(c).wait()
    interleave(dots_of(3), stats_units(2) + transpose_units(2, 4))
    d_copy(6).start()
    for c in (6, 7):
        h_copy(c).start()
    w_copy(1).start()
    send_sums(0)

    d_copy(4).wait()
    for c in (4, 5):
        h_copy(c).wait()
    w_copy(0).wait()
    interleave(dots_of(4), stats_units(3) + transpose_units(4, 6) + w2_units(0))
    d_copy(7).start()
    w_copy(2).start()
    finish_sums(0)

    d_copy(5).wait()
    for c in (6, 7):
        h_copy(c).wait()
    interleave(dots_of(5), stats_units(4) + transpose_units(6, 8) + scale_units(0))
    send_scalars(0) if False else None

    d_copy(6).wait()
    w_copy(1).wait()
    interleave(dots_of(6), stats_units(5) + w2_units(1))
    send_scalars(0)
    send_sums(1)

    d_copy(7).wait()
    w_copy(2).wait()
    interleave(dots_of(7), stats_units(6) + w2_units(2))
    finish_scalars(0)
    for unit in stats_units(7):
        unit()
    send_sums(2)
    finish_sums(1)
    for unit in scale_units(1):
        unit()
    send_scalars(1)
    finish_sums(2)
    for unit in scale_units(2):
        unit()
    send_scalars(2)
    finish_scalars(1)
    finish_scalars(2)

    for mat in range(3):
        row_copy(mat).wait_send()
        for d in (1, 2, 3):
            col_copy(mat, d).wait_send()
        for i in range(len(others)):
            scal_copy(mat, i).wait_send()


def update_kernel(
    hg, hu, hd, wg, wu, wd, kap, rg, cg, ru, cu, rd, cd,
    og, ou, od, rg_o, cg_o, ru_o, cu_o, rd_o, cd_o,
    sg, su, sd, sems,
):
    H, W, O, S = (hg, hu, hd), (wg, wu, wd), (og, ou, od), (sg, su, sd)
    n_sem = 0
    copies = []
    for mat in range(3):
        m, n = SHAPES[mat]
        k = kap[mat][0:1, 0:1]
        step = 64 if mat < 2 else 128
        for r in range(0, m, step):
            for c in range(0, n, 256):
                S[mat][r:r + step, c:c + 256] = (
                    W[mat][r:r + step, c:c + 256] - k * H[mat][r:r + step, c:c + 256])
            copy = pltpu.make_async_copy(S[mat].at[r:r + step, :], O[mat].at[r:r + step, :], sems.at[n_sem])
            copy.start()
            copies.append(copy)
            n_sem += 1
    for src, dst in ((rg, rg_o), (cg, cg_o), (ru, ru_o), (cu, cu_o), (rd, rd_o), (cd, cd_o)):
        dst[...] = src[...]
    for copy in copies:
        copy.wait()


def local_program(x_in, h_act, d_gate, d_up, d_out, w_gate, w_up, w_down, r_gate, c_gate, r_up, c_up, r_down, c_down, beta_two, rel_step, clip_thr):
    any_spec = pl.BlockSpec(memory_space=pl.ANY)
    vmem_spec = pl.BlockSpec(memory_space=pltpu.VMEM)
    smem_spec = pl.BlockSpec(memory_space=pltpu.SMEM)
    stat_shapes = [(n // LANES, LANES) for shape in SHAPES for n in shape]
    stats = [v.reshape(s) for v, s in zip((r_gate, c_gate, r_up, c_up, r_down, c_down), stat_shapes)]
    scalars = [v.reshape(1) for v in (beta_two, rel_step, clip_thr)]
    big = [pltpu.HBM] * 8

    outs = pl.pallas_call(
        stats_kernel,
        out_shape=[pltpu.VMEM(s, F32) for s in SHAPES] * 2 + [pltpu.VMEM(s, F32) for s in stat_shapes]
        + [pltpu.VMEM((3, 8, LANES), F32)],
        in_specs=[any_spec] * 8 + [vmem_spec] * 6 + [smem_spec] * 3,
        out_specs=[vmem_spec] * 13,
        scratch_shapes=[
            pltpu.VMEM((SLOTS, K, SLOT_WIDTH), BF16),
            pltpu.VMEM((K, 512), BF16),
            pltpu.VMEM((512, K), BF16),
            pltpu.VMEM((4, HCHUNK, 1408), BF16),
            pltpu.VMEM((1408, K), BF16),
            pltpu.VMEM((1408, LANES), F32),
        ] + [pltpu.VMEM((m, LANES), F32) for m, n in SHAPES]
        + [pltpu.VMEM((8, n), F32) for m, n in SHAPES]
        + [pltpu.VMEM((n // LANES, LANES), F32) for m, n in SHAPES]
        + [pltpu.VMEM((COLS, m // LANES, LANES), F32) for m, n in SHAPES]
        + [pltpu.VMEM((ROWS, n // LANES, LANES), F32) for m, n in SHAPES]
        + [
            pltpu.VMEM((3, ROWS * COLS, 8, LANES), F32),
            pltpu.VMEM((3, 8, LANES), F32),
            pltpu.VMEM((3, 8, LANES), F32),
            pltpu.SemaphoreType.DMA((SLOTS,)),
            pltpu.SemaphoreType.DMA((8,)),
            pltpu.SemaphoreType.DMA((4,)),
            pltpu.SemaphoreType.DMA((3,)),
            pltpu.SemaphoreType.DMA((3,)),
            pltpu.SemaphoreType.DMA((3,)),
            pltpu.SemaphoreType.DMA((3, 3)),
            pltpu.SemaphoreType.DMA((3, 3)),
            pltpu.SemaphoreType.DMA((3, 7)),
            pltpu.SemaphoreType.DMA((3, 7)),
        ],
        compiler_params=pltpu.CompilerParams(
            collective_id=0, has_side_effects=True, vmem_limit_bytes=29 * 1024 * 1024),
        name="stats",
    )(
        *[pltpu.with_memory_space_constraint(v, pltpu.HBM)
          for v in (x_in, h_act, d_gate, d_up, d_out, w_gate, w_up, w_down)],
        *stats, *scalars)

    H, W, new, kap = outs[0:3], outs[3:6], outs[6:12], outs[12]
    res = pl.pallas_call(
        update_kernel,
        out_shape=[jax.ShapeDtypeStruct(s, F32) for s in SHAPES]
        + [jax.ShapeDtypeStruct(s, F32) for s in stat_shapes],
        in_specs=[vmem_spec] * 13,
        out_specs=[any_spec] * 3 + [vmem_spec] * 6,
        scratch_shapes=[pltpu.VMEM(s, F32) for s in SHAPES] + [pltpu.SemaphoreType.DMA((27,))],
        compiler_params=pltpu.CompilerParams(vmem_limit_bytes=29 * 1024 * 1024),
        name="update",
    )(*[pltpu.with_memory_space_constraint(v, pltpu.VMEM) for v in (*H, *W, kap, *new)])
    flat = [v.reshape(-1) for v in res[3:]]
    return (*res[:3], *flat)


def solution(mesh):
    act_spec = P(None, "row")
    cot_spec = P(None, "col")
    w_spec = P("row", "col")
    r_spec = P("row")
    c_spec = P("col")
    s_spec = P()
    return jax.shard_map(local_program, mesh=mesh, in_specs=(act_spec, act_spec, cot_spec, cot_spec, cot_spec, w_spec, w_spec, w_spec, r_spec, c_spec, r_spec, c_spec, r_spec, c_spec, s_spec, s_spec, s_spec), out_specs=(w_spec, w_spec, w_spec, r_spec, c_spec, r_spec, c_spec, r_spec, c_spec), check_vma=False)
```

```python
import jax
import jax.numpy as jnp
from jax import lax
from jax.experimental import pallas as pl
from jax.experimental.pallas import tpu as pltpu
from jax.sharding import PartitionSpec as P

EPS_SQ = 1e-30
EPS_SCALE = 1e-3
LANES = 128
K = 2048
ROWS, COLS = 4, 2
F32 = jnp.float32
BF16 = jnp.bfloat16
MESH = pl.DeviceIdType.MESH

DOWN, GATE, UP = 0, 1, 2
SHAPES = ((1408, 1024), (512, 2816), (512, 2816))
TOTALS = tuple((m * ROWS, n * COLS) for m, n in SHAPES)
PIECES = ((0, 256), (256, 512), (512, 1024), (1024, 1536), (1536, 2048))
GATE_BLOCKS = ((0, 1024), (1024, 2048), (2048, 2816))
UP_BLOCKS = ((0, 512), (512, 1536), (1536, 2048), (2048, 2816))
BLOCKS = tuple((GATE, *b) for b in GATE_BLOCKS) + tuple((UP, *b) for b in UP_BLOCKS)
SLOT_OF = (1, 2, 0, 1, 2, 0, 1)
CHUNK = 64
OTHERS = [(dc, dr) for dc in range(COLS) for dr in range(ROWS) if (dc, dr) != (0, 0)]


def interleave(dots, units):
    done = 0
    for i, dot in enumerate(dots):
        dot()
        upto = len(units) * (i + 1) // len(dots)
        for unit in units[done:upto]:
            unit()
        done = upto
    for unit in units[done:]:
        unit()


def fold(x):
    return jnp.sum(x.reshape(x.shape[0] // 8, 8, x.shape[1]), axis=0)


def place():
    return lax.axis_index("data"), lax.axis_index("col"), lax.axis_index("row")


def peer(dc, dr):
    d, c, r = place()
    return (d, lax.rem(c + dc, COLS), lax.rem(r + dr, ROWS))


def signal_entry(barrier):
    for dc, dr in OTHERS:
        pl.semaphore_signal(barrier, inc=1, device_id=peer(dc, dr), device_id_type=MESH)


def scalar_copies(buf, send, recv):
    _, c, r = place()
    me = c * ROWS + r
    return [
        pltpu.make_async_remote_copy(
            src_ref=buf.at[me], dst_ref=buf.at[me], send_sem=send.at[i], recv_sem=recv.at[i],
            device_id=peer(*OTHERS[i]), device_id_type=MESH)
        for i in range(len(OTHERS))
    ]


def scalar_tile(s, w, r):
    rows = [jnp.sum(v, axis=0, keepdims=True) for v in (s, w, r)]
    return jnp.concatenate(rows + [jnp.zeros((5, LANES), F32)], axis=0)


def step_of(mat, buf, rel, clip):
    mt, nt = TOTALS[mat]
    tot = buf[0]
    for i in range(1, ROWS * COLS):
        tot = tot + buf[i]
    tot = jnp.sum(tot, axis=1, keepdims=True)
    s, w, r = tot[0:1, :], tot[1:2, :], tot[2:3, :]
    r_mean = r * (1.0 / (COLS * mt))
    u_rms = jnp.sqrt(s * (1.0 / (mt * nt)) * r_mean)
    w_rms = jnp.sqrt(w * (1.0 / (mt * nt)))
    step = rel * jnp.maximum(EPS_SCALE, w_rms)
    k = step * jnp.sqrt(r_mean) / jnp.maximum(1.0, u_rms / clip)
    return jnp.broadcast_to(k, (8, LANES))


def main_kernel(
    x_hbm, h_hbm, dg_hbm, du_hbm, do_hbm, wg_hbm, wu_hbm, wd_hbm,
    rg, cg, ru, cu, rd, cd, beta, rel, clip,
    gu, wu, wd, wg, rd_new, cd_new, rg_new, cg_new, ru_new, cu_new, kap,
    gd, gg, ring, xt, hs, ht, rowacc, abc_d, abc_g, abc_u, cacc_d, cacc_g, cacc_u,
    bv_d, bv_g, bv_u, rbuf_d, rbuf_g, rbuf_u, cbuf_d, cbuf_g, cbuf_u, sbuf, sacc, wacc,
    ring_sem, h_sem, w_sem, r_send, r_recv, c_send, c_recv, s_send, s_recv,
):
    G, W = (gd, gg, gu), (wd, wg, wu)
    d_hbm, w_hbm = (do_hbm, dg_hbm, du_hbm), (wd_hbm, wg_hbm, wu_hbm)
    r_old, c_old = (rd, rg, ru), (cd, cg, cu)
    r_new, c_new = (rd_new, rg_new, ru_new), (cd_new, cg_new, cu_new)
    abc, cacc, bv = (abc_d, abc_g, abc_u), (cacc_d, cacc_g, cacc_u), (bv_d, bv_g, bv_u)
    rbuf, cbuf = (rbuf_d, rbuf_g, rbuf_u), (cbuf_d, cbuf_g, cbuf_u)
    _, me_c, me_r = place()

    def piece_copies(p):
        ks = slice(*PIECES[p])
        return (
            pltpu.make_async_copy(h_hbm.at[ks, :], hs.at[ks, :], h_sem.at[0, p]),
            pltpu.make_async_copy(do_hbm.at[ks, :], ring.at[0, ks, :], h_sem.at[1, p]),
        )

    x_copy = pltpu.make_async_copy(x_hbm, ring.at[2, :, :512], h_sem.at[2, 0])

    def d_copy(j):
        mat, n0, n1 = BLOCKS[j]
        slot = SLOT_OF[j]
        return pltpu.make_async_copy(
            d_hbm[mat].at[:, n0:n1], ring.at[slot, :, : n1 - n0], ring_sem.at[j])

    def w_copy(mat):
        return pltpu.make_async_copy(w_hbm[mat], W[mat], w_sem.at[mat])

    def sum_copies(mat):
        row = pltpu.make_async_remote_copy(
            src_ref=rbuf[mat].at[me_c], dst_ref=rbuf[mat].at[me_c],
            send_sem=r_send.at[mat], recv_sem=r_recv.at[mat],
            device_id=peer(1, 0), device_id_type=MESH)
        cols = [
            pltpu.make_async_remote_copy(
                src_ref=cbuf[mat].at[me_r], dst_ref=cbuf[mat].at[me_r],
                send_sem=c_send.at[mat, d - 1], recv_sem=c_recv.at[mat, d - 1],
                device_id=peer(0, d), device_id_type=MESH)
            for d in (1, 2, 3)
        ]
        return [row, *cols]

    def tiles(mat):
        return scalar_copies(sbuf.at[mat], s_send.at[mat], s_recv.at[mat])

    def start(copies):
        for c in copies:
            c.start()

    def wait(copies):
        for c in copies:
            c.wait()

    def wait_recv(copies):
        for c in copies:
            c.wait_recv()

    def stats_units(mat, n0, n1):
        units = []
        for r in range(0, SHAPES[mat][0], CHUNK):
            def unit(r=r):
                part = None
                for t in range(n0 // LANES, n1 // LANES):
                    g = G[mat][r:r + CHUNK, t * LANES:(t + 1) * LANES]
                    q = g * g
                    part = q if part is None else part + q
                    col = fold(q)
                    cols = pl.ds(t * LANES, LANES)
                    cacc[mat][:, cols] = col if r == 0 else cacc[mat][:, cols] + col
                rows = pl.ds(r, CHUNK)
                rowacc[rows, :] = part if n0 == 0 else rowacc[rows, :] + part
            units.append(unit)
        return units

    def sums_units(mat):
        m, n = SHAPES[mat]
        units = []
        for i in range(m // LANES):
            def rows(i=i):
                block = rowacc[i * LANES:(i + 1) * LANES, :].T
                rbuf[mat][me_c, i:i + 1, :] = jnp.sum(block, axis=0, keepdims=True)
            units.append(rows)
        for t in range(n // LANES):
            def cols(t=t):
                cbuf[mat][me_r, t:t + 1, :] = jnp.sum(
                    cacc[mat][:, t * LANES:(t + 1) * LANES], axis=0, keepdims=True)
            units.append(cols)
        return units

    def w2_units(mat):
        units = []
        m, n = SHAPES[mat]
        acc_ref = wacc.at[mat]
        for r in range(0, m, CHUNK):
            def unit(r=r):
                acc = None
                for t in range(n // LANES):
                    w = W[mat][r:r + CHUNK, t * LANES:(t + 1) * LANES]
                    f = fold(w * w)
                    acc = f if acc is None else acc + f
                acc_ref[...] = acc if r == 0 else acc_ref[...] + acc
            units.append(unit)
        return units

    def factor_units(mat):
        m, n = SHAPES[mat]
        mt, nt = TOTALS[mat]

        def new():
            b2 = beta[0]
            rows = rbuf[mat][0] + rbuf[mat][1]
            cols = (cbuf[mat][0] + cbuf[mat][1]) + (cbuf[mat][2] + cbuf[mat][3])
            rn = b2 * r_old[mat][...] + (1.0 - b2) * (rows * (1.0 / nt) + EPS_SQ)
            cn = b2 * c_old[mat][...] + (1.0 - b2) * (cols * (1.0 / mt) + EPS_SQ)
            r_new[mat][...] = rn
            c_new[mat][...] = cn
            bv[mat][...] = lax.rsqrt(cn)

        units = [new]
        for i in range(m // LANES):
            def unit(i=i):
                a = lax.rsqrt(r_new[mat][i:i + 1, :])
                abc[mat][i * LANES:(i + 1) * LANES, :] = jnp.broadcast_to(a, (LANES, LANES)).T
            units.append(unit)
        return units

    def scale_units(mat):
        units = []
        m, n = SHAPES[mat]
        for r in range(0, m, CHUNK):
            def unit(r=r):
                acc = None
                a = abc[mat][r:r + CHUNK, :]
                for t in range(n // LANES):
                    cols = slice(t * LANES, (t + 1) * LANES)
                    h = G[mat][r:r + CHUNK, cols] * a * bv[mat][t:t + 1, :]
                    G[mat][r:r + CHUNK, cols] = h
                    f = fold(h * h)
                    acc = f if acc is None else acc + f
                sacc[mat] = acc if r == 0 else sacc[mat] + acc
            units.append(unit)
        return units

    def update_units(mat):
        def step():
            kap[mat] = step_of(mat, sbuf.at[mat], rel[0], clip[0])

        units = [step]
        m, n = SHAPES[mat]
        for r in range(0, m, CHUNK):
            def unit(r=r):
                k = kap[mat, 0:1, :]
                for t in range(n // LANES):
                    cols = slice(t * LANES, (t + 1) * LANES)
                    W[mat][r:r + CHUNK, cols] = W[mat][r:r + CHUNK, cols] - k * G[mat][r:r + CHUNK, cols]
            units.append(unit)
        return units

    def tile_unit(mat):
        def unit():
            _, c, r = place()
            sbuf[mat, c * ROWS + r] = scalar_tile(sacc[mat], wacc[mat], r_new[mat][...])
        return [unit]

    def h_units(p):
        k0, k1 = PIECES[p]
        units = []
        for k in range(k0, k1, 256):
            for i in range(0, SHAPES[DOWN][0], LANES):
                def unit(k=k, i=i):
                    ht[i:i + LANES, k:k + 256] = hs[k:k + 256, i:i + LANES].T
                units.append(unit)
        return units

    def x_units():
        units = []
        for k in range(0, K, 256):
            for i in range(0, 512, LANES):
                def unit(k=k, i=i):
                    xt[i:i + LANES, k:k + 256] = ring[2, k:k + 256, i:i + LANES].T
                units.append(unit)
        return units

    def down_dots(p):
        ks = slice(*PIECES[p])
        out = []
        for r in range(0, 1408, 352):
            for c in range(0, 1024, 512):
                def dot(r=r, c=c):
                    rs, cs = slice(r, r + 352), slice(c, c + 512)
                    part = jnp.dot(ht[rs, ks], ring[0, ks, cs], preferred_element_type=F32)
                    gd[rs, cs] = part if p == 0 else gd[rs, cs] + part
                out.append(dot)
        return out

    def dots_of(j):
        mat, n0, n1 = BLOCKS[j]
        slot = SLOT_OF[j]
        out = []

        def dot(r0, r1, c0, c1):
            def run():
                G[mat][r0:r1, n0 + c0:n0 + c1] = jnp.dot(
                    xt[r0:r1, :], ring[slot, :, c0:c1], preferred_element_type=F32)
            return run

        w = n1 - n0
        for c in range(0, w, 512):
            if c + 512 <= w:
                out.append(dot(0, 512, c, c + 512))
            else:
                out += [dot(0, 256, c, w), dot(256, 512, c, w)]
        return out

    def run(units):
        for unit in units:
            unit()

    for p in (0, 1, 2):
        start(piece_copies(p))
    barrier = pltpu.get_barrier_semaphore()
    signal_entry(barrier)
    wait(piece_copies(0))
    start(piece_copies(3))
    start(piece_copies(4))
    x_copy.start()
    run(h_units(0))
    for p in range(4):
        wait(piece_copies(p + 1))
        if p == 2:
            d_copy(0).start()
            w_copy(DOWN).start()
        interleave(down_dots(p), h_units(p + 1))
    x_copy.wait()
    interleave(down_dots(4), x_units())
    d_copy(1).start()
    d_copy(2).start()

    d_copy(0).wait()
    interleave(dots_of(0), stats_units(DOWN, 0, 1024) + sums_units(DOWN))
    pl.semaphore_wait(barrier, len(OTHERS))
    start(sum_copies(DOWN))
    d_copy(3).start()
    w_copy(GATE).start()

    d_copy(1).wait()
    w_copy(DOWN).wait()
    interleave(dots_of(1), stats_units(GATE, 0, 1024) + w2_units(DOWN))
    d_copy(4).start()

    d_copy(2).wait()
    wait_recv(sum_copies(DOWN))
    interleave(dots_of(2), factor_units(DOWN) + scale_units(DOWN) + tile_unit(DOWN) + stats_units(GATE, 1024, 2048))
    start(tiles(DOWN))
    d_copy(5).start()
    w_copy(UP).start()

    d_copy(3).wait()
    interleave(dots_of(3), stats_units(GATE, 2048, 2816) + sums_units(GATE))
    start(sum_copies(GATE))
    d_copy(6).start()

    d_copy(4).wait()
    w_copy(GATE).wait()
    wait_recv(tiles(DOWN))
    interleave(dots_of(4), stats_units(UP, 0, 512) + w2_units(GATE) + update_units(DOWN)[:12])

    d_copy(5).wait()
    wait_recv(sum_copies(GATE))
    interleave(dots_of(5), factor_units(GATE) + scale_units(GATE) + tile_unit(GATE))
    start(tiles(GATE))

    d_copy(6).wait()
    w_copy(UP).wait()
    interleave(dots_of(6), update_units(DOWN)[12:] + stats_units(UP, 512, 1536) + stats_units(UP, 1536, 2048) + w2_units(UP))

    run(stats_units(UP, 2048, 2816) + sums_units(UP))
    start(sum_copies(UP))
    wait_recv(tiles(GATE))
    run(update_units(GATE))
    wait_recv(sum_copies(UP))
    run(factor_units(UP) + scale_units(UP) + tile_unit(UP))
    start(tiles(UP))
    for mat in range(3):
        for c in sum_copies(mat):
            c.wait_send()
    wait_recv(tiles(UP))
    kap[UP] = step_of(UP, sbuf.at[UP], rel[0], clip[0])
    for mat in range(3):
        for c in tiles(mat):
            c.wait_send()


def update_kernel(
    gu, wu, wd, wg, rd, cd, rg, cg, ru, cu, kap,
    wu_o, wd_o, wg_o, rd_o, cd_o, rg_o, cg_o, ru_o, cu_o, stage, sems, up_sems,
):
    srcs = (wd, wg, rd, cd, rg, cg, ru, cu)
    dsts = (wd_o, wg_o, rd_o, cd_o, rg_o, cg_o, ru_o, cu_o)
    copies = [pltpu.make_async_copy(src, dst, sems.at[i]) for i, (src, dst) in enumerate(zip(srcs, dsts))]
    for c in copies:
        c.start()
    m, n = SHAPES[UP]
    k = kap[UP, 0:1, :]
    for i, r in enumerate(range(0, m, CHUNK)):
        for t in range(n // LANES):
            cols = slice(t * LANES, (t + 1) * LANES)
            stage[r:r + CHUNK, cols] = wu[r:r + CHUNK, cols] - k * gu[r:r + CHUNK, cols]
        copies.append(pltpu.make_async_copy(stage.at[r:r + CHUNK, :], wu_o.at[r:r + CHUNK, :], up_sems.at[i]))
        copies[-1].start()
    for copy in copies:
        copy.wait()


VMEM_LIMIT = 41 * 1024 * 1024


def local_program(x_in, h_act, d_gate, d_up, d_out, w_gate, w_up, w_down, r_gate, c_gate, r_up, c_up, r_down, c_down, beta_two, rel_step, clip_thr):
    any_spec = pl.BlockSpec(memory_space=pl.ANY)
    vmem_spec = pl.BlockSpec(memory_space=pltpu.VMEM)
    smem_spec = pl.BlockSpec(memory_space=pltpu.SMEM)

    def stat_shape(v):
        return (v // LANES, LANES)

    stats = [v.reshape(stat_shape(v.shape[0])) for v in (r_gate, c_gate, r_up, c_up, r_down, c_down)]
    beta, rel, clip = [v.reshape(1) for v in (beta_two, rel_step, clip_thr)]
    rows = [stat_shape(m) for m, n in SHAPES]
    cols = [stat_shape(n) for m, n in SHAPES]
    dma = pltpu.SemaphoreType.DMA

    stat_pairs = [s for pair in zip(rows, cols) for s in pair]
    outs = pl.pallas_call(
        main_kernel,
        out_shape=[pltpu.VMEM(SHAPES[UP], F32)] * 2 + [pltpu.VMEM(s, F32) for s in SHAPES[:2]]
        + [pltpu.VMEM(s, F32) for s in stat_pairs] + [pltpu.VMEM((3, 8, LANES), F32)],
        in_specs=[any_spec] * 8 + [vmem_spec] * 6 + [smem_spec] * 3,
        out_specs=[vmem_spec] * 11,
        scratch_shapes=[
            pltpu.VMEM(SHAPES[DOWN], F32),
            pltpu.VMEM(SHAPES[GATE], F32),
            pltpu.VMEM((3, K, 1024), BF16),
            pltpu.VMEM((512, K), BF16),
            pltpu.VMEM((K, 1408), BF16),
            pltpu.VMEM((1408, K), BF16),
            pltpu.VMEM((1408, LANES), F32),
            pltpu.VMEM((1408, LANES), F32),
            pltpu.VMEM((512, LANES), F32),
            pltpu.VMEM((512, LANES), F32),
        ]
        + [pltpu.VMEM((8, n), F32) for m, n in SHAPES]
        + [pltpu.VMEM(s, F32) for s in cols]
        + [pltpu.VMEM((COLS, *s), F32) for s in rows]
        + [pltpu.VMEM((ROWS, *s), F32) for s in cols]
        + [
            pltpu.VMEM((3, ROWS * COLS, 8, LANES), F32),
            pltpu.VMEM((3, 8, LANES), F32),
            pltpu.VMEM((3, 8, LANES), F32),
            dma((7,)), dma((3, 5)), dma((3,)), dma((3,)), dma((3,)),
            dma((3, 3)), dma((3, 3)), dma((3, 7)), dma((3, 7)),
        ],
        compiler_params=pltpu.CompilerParams(
            collective_id=0, has_side_effects=True, vmem_limit_bytes=VMEM_LIMIT),
        name="main",
    )(
        *[pltpu.with_memory_space_constraint(v, pltpu.HBM)
          for v in (x_in, h_act, d_gate, d_up, d_out, w_gate, w_up, w_down)],
        *stats, beta, rel, clip)
    held = [pltpu.with_memory_space_constraint(v, pltpu.VMEM) for v in outs]
    res = pl.pallas_call(
        update_kernel,
        out_shape=[jax.ShapeDtypeStruct(s, F32) for s in (SHAPES[UP], *SHAPES[:2], *stat_pairs)],
        in_specs=[vmem_spec] * 11,
        out_specs=[any_spec] * 9,
        scratch_shapes=[pltpu.VMEM(SHAPES[UP], F32), dma((8,)), dma((8,))],
        compiler_params=pltpu.CompilerParams(vmem_limit_bytes=VMEM_LIMIT),
        name="update",
    )(*held)
    up, down, gate, rd_n, cd_n, rg_n, cg_n, ru_n, cu_n = res
    flat = [v.reshape(-1) for v in (rg_n, cg_n, ru_n, cu_n, rd_n, cd_n)]
    return (gate, up, down, *flat)


def solution(mesh):
    act_spec = P(None, "row")
    cot_spec = P(None, "col")
    w_spec = P("row", "col")
    r_spec = P("row")
    c_spec = P("col")
    s_spec = P()
    return jax.shard_map(local_program, mesh=mesh, in_specs=(act_spec, act_spec, cot_spec, cot_spec, cot_spec, w_spec, w_spec, w_spec, r_spec, c_spec, r_spec, c_spec, r_spec, c_spec, s_spec, s_spec, s_spec), out_specs=(w_spec, w_spec, w_spec, r_spec, c_spec, r_spec, c_spec, r_spec, c_spec), check_vma=False)
```

```python
import jax
import jax.numpy as jnp
from jax import lax
from jax.experimental import pallas as pl
from jax.experimental.pallas import tpu as pltpu
from jax.sharding import PartitionSpec as P

EPS_SQ = 1e-30
EPS_SCALE = 1e-3
LANES = 128
K = 2048
ROWS, COLS = 4, 2
F32 = jnp.float32
BF16 = jnp.bfloat16
MESH = pl.DeviceIdType.MESH

DOWN, GATE, UP = 0, 1, 2
SHAPES = ((1408, 1024), (512, 2816), (512, 2816))
TOTALS = tuple((m * ROWS, n * COLS) for m, n in SHAPES)
PIECES = ((0, 256), (256, 512), (512, 1024), (1024, 1536), (1536, 2048))
GATE_BLOCKS = ((0, 1024), (1024, 2048), (2048, 2816))
UP_BLOCKS = ((0, 512), (512, 1536), (1536, 2048), (2048, 2816))
BLOCKS = tuple((GATE, *b) for b in GATE_BLOCKS) + tuple((UP, *b) for b in UP_BLOCKS)
EARLY_COLS = 16
CHUNK = 64
OTHERS = [(dc, dr) for dc in range(COLS) for dr in range(ROWS) if (dc, dr) != (0, 0)]


def interleave(dots, units):
    done = 0
    for i, dot in enumerate(dots):
        upto = len(units) * (i + 1) // len(dots)
        for unit in units[done:upto]:
            unit()
        done = upto
        dot()


def fold(x):
    return jnp.sum(x.reshape(x.shape[0] // 8, 8, x.shape[1]), axis=0)


def place():
    return lax.axis_index("data"), lax.axis_index("col"), lax.axis_index("row")


def peer(dc, dr):
    d, c, r = place()
    return (d, lax.rem(c + dc, COLS), lax.rem(r + dr, ROWS))


def signal_entry(barrier):
    for dc, dr in OTHERS:
        pl.semaphore_signal(barrier, inc=1, device_id=peer(dc, dr), device_id_type=MESH)


def scalar_copies(buf, send, recv):
    _, c, r = place()
    me = c * ROWS + r
    return [
        pltpu.make_async_remote_copy(
            src_ref=buf.at[me], dst_ref=buf.at[me], send_sem=send.at[i], recv_sem=recv.at[i],
            device_id=peer(*OTHERS[i]), device_id_type=MESH)
        for i in range(len(OTHERS))
    ]


def scalar_tile(s, w, r):
    rows = [jnp.sum(v, axis=0, keepdims=True) for v in (s, w, r)]
    return jnp.concatenate(rows + [jnp.zeros((5, LANES), F32)], axis=0)


def step_of(mat, buf, rel, clip):
    mt, nt = TOTALS[mat]
    tot = buf[0]
    for i in range(1, ROWS * COLS):
        tot = tot + buf[i]
    tot = jnp.sum(tot, axis=1, keepdims=True)
    s, w, r = tot[0:1, :], tot[1:2, :], tot[2:3, :]
    r_mean = r * (1.0 / (COLS * mt))
    u_rms = jnp.sqrt(s * (1.0 / (mt * nt)) * r_mean)
    w_rms = jnp.sqrt(w * (1.0 / (mt * nt)))
    step = rel * jnp.maximum(EPS_SCALE, w_rms)
    k = step * jnp.sqrt(r_mean) / jnp.maximum(1.0, u_rms / clip)
    return jnp.broadcast_to(k, (8, LANES))


def main_kernel(
    x_hbm, h_hbm, dg_hbm, du_hbm, do_hbm, wg_hbm, wu_hbm, wd_hbm,
    rg_hbm, cg_hbm, ru_hbm, cu_hbm, rd_hbm, cd_hbm, beta, rel, clip,
    gu, wu, wd, wg, rd_new, cd_new, rg_new, cg_new, ru_new, cu_new, kap, abc_u, bv_u,
    gd, gg, ring, xt, hs, ht, rowacc, abc_d, abc_g, cacc_d, cacc_g, cacc_u,
    bv_d, bv_g, rd, cd, rg, cg, ru, cu, rbuf_d, rbuf_g, rbuf_u, cbuf_d, cbuf_g, cbuf_u, sbuf, sacc, wacc,
    ring_sem, h_sem, w_sem, old_sem, r_send, r_recv, c_send, c_recv, s_send, s_recv,
):
    G, W = (gd, gg, gu), (wd, wg, wu)
    d_hbm, w_hbm = (do_hbm, dg_hbm, du_hbm), (wd_hbm, wg_hbm, wu_hbm)
    r_old, c_old = (rd, rg, ru), (cd, cg, cu)
    r_new, c_new = (rd_new, rg_new, ru_new), (cd_new, cg_new, cu_new)
    abc, cacc, bv = (abc_d, abc_g, abc_u), (cacc_d, cacc_g, cacc_u), (bv_d, bv_g, bv_u)
    rbuf, cbuf = (rbuf_d, rbuf_g, rbuf_u), (cbuf_d, cbuf_g, cbuf_u)
    _, me_c, me_r = place()

    def piece_copies(p):
        ks = slice(*PIECES[p])
        return (
            pltpu.make_async_copy(h_hbm.at[ks, :], hs.at[ks, :], h_sem.at[0, p]),
            pltpu.make_async_copy(do_hbm.at[ks, :], ring.at[0, ks, :], h_sem.at[1, p]),
        )

    x_copy = pltpu.make_async_copy(x_hbm, ring.at[2, :, :512], h_sem.at[2, 0])

    places = (
        ring.at[1], hs.at[:, :1024], ring.at[2, :, :768],
        ring.at[0, :, :512], ring.at[1], ring.at[0, :, 512:1024], hs.at[:, :768],
    )

    def d_copy(j):
        mat, n0, n1 = BLOCKS[j]
        return pltpu.make_async_copy(d_hbm[mat].at[:, n0:n1], places[j], ring_sem.at[j])

    old_copies = [
        pltpu.make_async_copy(src, dst, old_sem.at[i])
        for i, (src, dst) in enumerate(zip((rd_hbm, cd_hbm, rg_hbm, cg_hbm, ru_hbm, cu_hbm), (rd, cd, rg, cg, ru, cu)))
    ]

    def w_copy(mat):
        return pltpu.make_async_copy(w_hbm[mat], W[mat], w_sem.at[mat])

    def col_copies(mat, part, sem):
        return [
            pltpu.make_async_remote_copy(
                src_ref=cbuf[mat].at[me_r, part], dst_ref=cbuf[mat].at[me_r, part],
                send_sem=c_send.at[sem, d - 1], recv_sem=c_recv.at[sem, d - 1],
                device_id=peer(0, d), device_id_type=MESH)
            for d in (1, 2, 3)
        ]

    early = col_copies(UP, slice(0, EARLY_COLS), 3)

    def sum_copies(mat):
        row = pltpu.make_async_remote_copy(
            src_ref=rbuf[mat].at[me_c], dst_ref=rbuf[mat].at[me_c],
            send_sem=r_send.at[mat], recv_sem=r_recv.at[mat],
            device_id=peer(1, 0), device_id_type=MESH)
        return [row, *col_copies(mat, slice(EARLY_COLS if mat == UP else 0, SHAPES[mat][1] // LANES), mat)]

    def tiles(mat):
        return scalar_copies(sbuf.at[mat], s_send.at[mat], s_recv.at[mat])

    def start(copies):
        for c in copies:
            c.start()

    def wait(copies):
        for c in copies:
            c.wait()

    def wait_recv(copies):
        for c in copies:
            c.wait_recv()

    def stats_units(mat, n0, n1):
        units = []
        for r in range(0, SHAPES[mat][0], CHUNK):
            def unit(r=r):
                part = None
                for t in range(n0 // LANES, n1 // LANES):
                    g = G[mat][r:r + CHUNK, t * LANES:(t + 1) * LANES]
                    q = g * g
                    part = q if part is None else part + q
                    col = fold(q)
                    cols = pl.ds(t * LANES, LANES)
                    cacc[mat][:, cols] = col if r == 0 else cacc[mat][:, cols] + col
                rows = pl.ds(r, CHUNK)
                rowacc[rows, :] = part if n0 == 0 else rowacc[rows, :] + part
            units.append(unit)
        return units

    def row_units(mat):
        units = []
        for i in range(SHAPES[mat][0] // LANES):
            def rows(i=i):
                block = rowacc[i * LANES:(i + 1) * LANES, :].T
                rbuf[mat][me_c, i:i + 1, :] = jnp.sum(block, axis=0, keepdims=True)
            units.append(rows)
        return units

    def col_units(mat, t0, t1):
        units = []
        for t in range(t0, t1):
            def cols(t=t):
                cbuf[mat][me_r, t:t + 1, :] = jnp.sum(
                    cacc[mat][:, t * LANES:(t + 1) * LANES], axis=0, keepdims=True)
            units.append(cols)
        return units

    def sums_units(mat):
        return row_units(mat) + col_units(mat, 0, SHAPES[mat][1] // LANES)

    def w2_units(mat):
        units = []
        m, n = SHAPES[mat]
        for i in range(m // CHUNK):
            def unit(i=i):
                acc = None
                for t in range(n // LANES):
                    w = W[mat][i * CHUNK:(i + 1) * CHUNK, t * LANES:(t + 1) * LANES]
                    f = fold(w * w)
                    acc = f if acc is None else acc + f
                wacc[mat, i] = acc
            units.append(unit)
        return units

    def factor_units(mat):
        m, n = SHAPES[mat]
        mt, nt = TOTALS[mat]

        def new():
            b2 = beta[0]
            rows = rbuf[mat][0] + rbuf[mat][1]
            cols = (cbuf[mat][0] + cbuf[mat][1]) + (cbuf[mat][2] + cbuf[mat][3])
            rn = b2 * r_old[mat][...] + (1.0 - b2) * (rows * (1.0 / nt) + EPS_SQ)
            cn = b2 * c_old[mat][...] + (1.0 - b2) * (cols * (1.0 / mt) + EPS_SQ)
            r_new[mat][...] = rn
            c_new[mat][...] = cn
            bv[mat][...] = lax.rsqrt(cn)

        units = [new]
        for i in range(m // LANES):
            def unit(i=i):
                a = lax.rsqrt(r_new[mat][i:i + 1, :])
                abc[mat][i * LANES:(i + 1) * LANES, :] = jnp.broadcast_to(a, (LANES, LANES)).T
            units.append(unit)
        return units

    def scale_units(mat):
        units = []
        m, n = SHAPES[mat]
        for i in range(m // CHUNK):
            def unit(i=i):
                acc = None
                rows = slice(i * CHUNK, (i + 1) * CHUNK)
                a = abc[mat][rows, :]
                for t in range(n // LANES):
                    h = G[mat][rows, t * LANES:(t + 1) * LANES] * a * bv[mat][t:t + 1, :]
                    f = fold(h * h)
                    acc = f if acc is None else acc + f
                sacc[mat, i] = acc
            units.append(unit)
        return units

    def update_units(mat):
        def step():
            kap[mat] = step_of(mat, sbuf.at[mat], rel[0], clip[0])

        units = [step]
        m, n = SHAPES[mat]
        for r in range(0, m, CHUNK):
            def unit(r=r):
                ka = abc[mat][r:r + CHUNK, :] * kap[mat, 0:1, :]
                for t in range(n // LANES):
                    cols = slice(t * LANES, (t + 1) * LANES)
                    W[mat][r:r + CHUNK, cols] = (
                        W[mat][r:r + CHUNK, cols] - G[mat][r:r + CHUNK, cols] * ka * bv[mat][t:t + 1, :])
            units.append(unit)
        return units

    def tile_unit(mat):
        def unit():
            _, c, r = place()
            chunks = SHAPES[mat][0] // CHUNK
            sbuf[mat, c * ROWS + r] = scalar_tile(
                jnp.sum(sacc[mat, :chunks], axis=0), jnp.sum(wacc[mat, :chunks], axis=0), r_new[mat][...])
        return [unit]

    def h_units(p):
        k0, k1 = PIECES[p]
        units = []
        for k in range(k0, k1, 256):
            for i in range(0, SHAPES[DOWN][0], LANES):
                def unit(k=k, i=i):
                    ht[i:i + LANES, k:k + 256] = hs[k:k + 256, i:i + LANES].T
                units.append(unit)
        return units

    def x_units():
        units = []
        for k in range(0, K, 256):
            for i in range(0, 512, LANES):
                def unit(k=k, i=i):
                    xt[i:i + LANES, k:k + 256] = ring[2, k:k + 256, i:i + LANES].T
                units.append(unit)
        return units

    def down_dots(p):
        ks = slice(*PIECES[p])
        out = []
        for r in range(0, 1408, 352):
            for c in range(0, 1024, 512):
                def dot(r=r, c=c):
                    rs, cs = slice(r, r + 352), slice(c, c + 512)
                    part = jnp.dot(ht[rs, ks], ring[0, ks, cs], preferred_element_type=F32)
                    gd[rs, cs] = part if p == 0 else gd[rs, cs] + part
                out.append(dot)
        return out

    def dots_of(j):
        mat, n0, n1 = BLOCKS[j]
        out = []

        def dot(r0, r1, c0, c1):
            def run():
                G[mat][r0:r1, n0 + c0:n0 + c1] = jnp.dot(
                    xt[r0:r1, :], places[j][:, c0:c1], preferred_element_type=F32)
            return run

        w = n1 - n0
        for c in range(0, w, 512):
            if c + 512 <= w:
                out.append(dot(0, 512, c, c + 512))
            else:
                out += [dot(0, 256, c, w), dot(256, 512, c, w)]
        return out

    def run(units):
        for unit in units:
            unit()

    for p in (0, 1, 2):
        start(piece_copies(p))
    start(old_copies)
    barrier = pltpu.get_barrier_semaphore()
    signal_entry(barrier)
    wait(piece_copies(0))
    start(piece_copies(3))
    start(piece_copies(4))
    x_copy.start()
    run(h_units(0))
    for p in range(4):
        wait(piece_copies(p + 1))
        if p == 1:
            d_copy(0).start()
        interleave(down_dots(p), h_units(p + 1))
    d_copy(1).start()
    x_copy.wait()
    interleave(down_dots(4), x_units())
    d_copy(2).start()
    w_copy(DOWN).start()
    d_copy(3).start()
    d_copy(5).start()

    d_copy(0).wait()
    wait(old_copies)
    interleave(dots_of(0), stats_units(DOWN, 0, 1024) + sums_units(DOWN))
    pl.semaphore_wait(barrier, len(OTHERS))
    start(sum_copies(DOWN))
    d_copy(4).start()
    w_copy(GATE).start()

    d_copy(1).wait()
    d_copy(2).wait()
    w_copy(DOWN).wait()
    interleave(dots_of(1), stats_units(GATE, 0, 1024) + w2_units(DOWN)[:11])
    interleave(dots_of(2), w2_units(DOWN)[11:] + stats_units(GATE, 1024, 2048))
    d_copy(6).start()
    w_copy(UP).start()

    d_copy(3).wait()
    interleave(dots_of(3), stats_units(GATE, 2048, 2816) + sums_units(GATE))
    start(sum_copies(GATE))

    d_copy(4).wait()
    d_copy(5).wait()
    w_copy(GATE).wait()
    wait_recv(sum_copies(DOWN))
    interleave(dots_of(4), factor_units(DOWN) + scale_units(DOWN) + stats_units(UP, 0, 512))
    interleave(dots_of(5), tile_unit(DOWN) + w2_units(GATE) + stats_units(UP, 512, 1536))
    start(tiles(DOWN))

    d_copy(6).wait()
    wait_recv(sum_copies(GATE))
    interleave(
        dots_of(6),
        factor_units(GATE) + scale_units(GATE) + tile_unit(GATE) + stats_units(UP, 1536, 2048)
        + col_units(UP, 0, EARLY_COLS))
    start(tiles(GATE))
    start(early)

    run(stats_units(UP, 2048, 2816) + row_units(UP) + col_units(UP, EARLY_COLS, 22))
    start(sum_copies(UP))
    w_copy(UP).wait()
    run(w2_units(UP))
    wait_recv(tiles(DOWN))
    run(update_units(DOWN))
    wait_recv(early)
    wait_recv(sum_copies(UP))
    run(factor_units(UP) + scale_units(UP) + tile_unit(UP))
    start(tiles(UP))
    wait_recv(tiles(GATE))
    run(update_units(GATE))
    for copies in [sum_copies(mat) for mat in range(3)] + [early, tiles(DOWN), tiles(GATE), tiles(UP)]:
        for c in copies:
            c.wait_send()
    wait_recv(tiles(UP))
    kap[UP] = step_of(UP, sbuf.at[UP], rel[0], clip[0])


def update_kernel(
    gu, wu, wd, wg, rd, cd, rg, cg, ru, cu, kap, abc, bv,
    wu_o, wd_o, wg_o, rd_o, cd_o, rg_o, cg_o, ru_o, cu_o, stage, sems, up_sems,
):
    srcs = (wd, wg, rd, cd, rg, cg, ru, cu)
    dsts = (wd_o, wg_o, rd_o, cd_o, rg_o, cg_o, ru_o, cu_o)
    copies = [pltpu.make_async_copy(src, dst, sems.at[i]) for i, (src, dst) in enumerate(zip(srcs, dsts))]
    for c in copies:
        c.start()
    m, n = SHAPES[UP]
    k = kap[UP, 0:1, :]
    for i, r in enumerate(range(0, m, CHUNK)):
        ka = abc[r:r + CHUNK, :] * k
        for t in range(n // LANES):
            cols = slice(t * LANES, (t + 1) * LANES)
            stage[r:r + CHUNK, cols] = wu[r:r + CHUNK, cols] - gu[r:r + CHUNK, cols] * ka * bv[t:t + 1, :]
        copies.append(pltpu.make_async_copy(stage.at[r:r + CHUNK, :], wu_o.at[r:r + CHUNK, :], up_sems.at[i]))
        copies[-1].start()
    for copy in copies:
        copy.wait()


VMEM_LIMIT = 41 * 1024 * 1024


def local_program(x_in, h_act, d_gate, d_up, d_out, w_gate, w_up, w_down, r_gate, c_gate, r_up, c_up, r_down, c_down, beta_two, rel_step, clip_thr):
    any_spec = pl.BlockSpec(memory_space=pl.ANY)
    vmem_spec = pl.BlockSpec(memory_space=pltpu.VMEM)
    smem_spec = pl.BlockSpec(memory_space=pltpu.SMEM)

    def stat_shape(v):
        return (v // LANES, LANES)

    stats = [v.reshape(stat_shape(v.shape[0])) for v in (r_gate, c_gate, r_up, c_up, r_down, c_down)]
    beta, rel, clip = [v.reshape(1) for v in (beta_two, rel_step, clip_thr)]
    rows = [stat_shape(m) for m, n in SHAPES]
    cols = [stat_shape(n) for m, n in SHAPES]
    dma = pltpu.SemaphoreType.DMA

    stat_pairs = [s for pair in zip(rows, cols) for s in pair]
    outs = pl.pallas_call(
        main_kernel,
        out_shape=[pltpu.VMEM(SHAPES[UP], F32)] * 2 + [pltpu.VMEM(s, F32) for s in SHAPES[:2]]
        + [pltpu.VMEM(s, F32) for s in stat_pairs]
        + [pltpu.VMEM((3, 8, LANES), F32), pltpu.VMEM((512, LANES), F32), pltpu.VMEM(cols[UP], F32)],
        in_specs=[any_spec] * 14 + [smem_spec] * 3,
        out_specs=[vmem_spec] * 13,
        scratch_shapes=[
            pltpu.VMEM(SHAPES[DOWN], F32),
            pltpu.VMEM(SHAPES[GATE], F32),
            pltpu.VMEM((3, K, 1024), BF16),
            pltpu.VMEM((512, K), BF16),
            pltpu.VMEM((K, 1408), BF16),
            pltpu.VMEM((1408, K), BF16),
            pltpu.VMEM((1408, LANES), F32),
            pltpu.VMEM((1408, LANES), F32),
            pltpu.VMEM((512, LANES), F32),
        ]
        + [pltpu.VMEM((8, n), F32) for m, n in SHAPES]
        + [pltpu.VMEM(s, F32) for s in cols[:2]]
        + [pltpu.VMEM(s, F32) for s in stat_pairs]
        + [pltpu.VMEM((COLS, *s), F32) for s in rows]
        + [pltpu.VMEM((ROWS, *s), F32) for s in cols]
        + [
            pltpu.VMEM((3, ROWS * COLS, 8, LANES), F32),
            pltpu.VMEM((3, 22, 8, LANES), F32),
            pltpu.VMEM((3, 22, 8, LANES), F32),
            dma((7,)), dma((3, 5)), dma((3,)), dma((6,)), dma((3,)), dma((3,)),
            dma((4, 3)), dma((4, 3)), dma((3, 7)), dma((3, 7)),
        ],
        compiler_params=pltpu.CompilerParams(
            collective_id=0, has_side_effects=True, vmem_limit_bytes=VMEM_LIMIT),
        name="main",
    )(
        *[pltpu.with_memory_space_constraint(v, pltpu.HBM)
          for v in (x_in, h_act, d_gate, d_up, d_out, w_gate, w_up, w_down, *stats)],
        beta, rel, clip)
    held = [pltpu.with_memory_space_constraint(v, pltpu.VMEM) for v in outs]
    res = pl.pallas_call(
        update_kernel,
        out_shape=[jax.ShapeDtypeStruct(s, F32) for s in (SHAPES[UP], *SHAPES[:2], *stat_pairs)],
        in_specs=[vmem_spec] * 13,
        out_specs=[any_spec] * 9,
        scratch_shapes=[pltpu.VMEM(SHAPES[UP], F32), dma((8,)), dma((8,))],
        compiler_params=pltpu.CompilerParams(vmem_limit_bytes=VMEM_LIMIT),
        name="update",
    )(*held)
    up, down, gate, rd_n, cd_n, rg_n, cg_n, ru_n, cu_n = res
    flat = [v.reshape(-1) for v in (rg_n, cg_n, ru_n, cu_n, rd_n, cd_n)]
    return (gate, up, down, *flat)


def solution(mesh):
    act_spec = P(None, "row")
    cot_spec = P(None, "col")
    w_spec = P("row", "col")
    r_spec = P("row")
    c_spec = P("col")
    s_spec = P()
    return jax.shard_map(local_program, mesh=mesh, in_specs=(act_spec, act_spec, cot_spec, cot_spec, cot_spec, w_spec, w_spec, w_spec, r_spec, c_spec, r_spec, c_spec, r_spec, c_spec, s_spec, s_spec, s_spec), out_specs=(w_spec, w_spec, w_spec, r_spec, c_spec, r_spec, c_spec, r_spec, c_spec), check_vma=False)
```

```python
import jax
import jax.numpy as jnp
from jax import lax
from jax.experimental import pallas as pl
from jax.experimental.pallas import tpu as pltpu
from jax.sharding import PartitionSpec as P

EPS_SQ = 1e-30
EPS_SCALE = 1e-3
LANES = 128
K = 2048
ROWS, COLS = 4, 2
F32 = jnp.float32
BF16 = jnp.bfloat16
MESH = pl.DeviceIdType.MESH

DOWN, GATE, UP = 0, 1, 2
SHAPES = ((1408, 1024), (512, 2816), (512, 2816))
TOTALS = tuple((m * ROWS, n * COLS) for m, n in SHAPES)
PIECES = ((0, 256), (256, 512), (512, 1024), (1024, 1536), (1536, 2048))
GATE_BLOCKS = ((0, 1024), (1024, 2048), (2048, 2816))
UP_BLOCKS = ((0, 512), (512, 1536), (1536, 2048), (2048, 2816))
BLOCKS = tuple((GATE, *b) for b in GATE_BLOCKS) + tuple((UP, *b) for b in UP_BLOCKS)
EARLY_COLS = 16
CHUNK = 64
OTHERS = [(dc, dr) for dc in range(COLS) for dr in range(ROWS) if (dc, dr) != (0, 0)]


def interleave(dots, units):
    done = 0
    for i, dot in enumerate(dots):
        upto = len(units) * (i + 1) // len(dots)
        for unit in units[done:upto]:
            unit()
        done = upto
        dot()


def fold(x):
    return jnp.sum(x.reshape(x.shape[0] // 8, 8, x.shape[1]), axis=0)


def place():
    return lax.axis_index("data"), lax.axis_index("col"), lax.axis_index("row")


def peer(dc, dr):
    d, c, r = place()
    return (d, lax.rem(c + dc, COLS), lax.rem(r + dr, ROWS))


def signal_entry(barrier):
    for dc, dr in OTHERS:
        pl.semaphore_signal(barrier, inc=1, device_id=peer(dc, dr), device_id_type=MESH)


def remote(ref, send, recv, to):
    return pltpu.make_async_remote_copy(
        src_ref=ref, dst_ref=ref, send_sem=send, recv_sem=recv, device_id=to, device_id_type=MESH)


def scalar_tile(s, w, r):
    rows = [jnp.sum(v, axis=0, keepdims=True) for v in (s, w, r)]
    return jnp.concatenate(rows + [jnp.zeros((1, LANES), F32)], axis=0)


def step_of(mat, buf, rel, clip):
    mt, nt = TOTALS[mat]
    tot = buf[0]
    for i in range(1, ROWS * COLS):
        tot = tot + buf[i]
    tot = jnp.sum(tot, axis=1, keepdims=True)
    s, w, r = tot[0:1, :], tot[1:2, :], tot[2:3, :]
    r_mean = r * (1.0 / (COLS * mt))
    u_rms = jnp.sqrt(s * (1.0 / (mt * nt)) * r_mean)
    w_rms = jnp.sqrt(w * (1.0 / (mt * nt)))
    step = rel * jnp.maximum(EPS_SCALE, w_rms)
    k = step * jnp.sqrt(r_mean) / jnp.maximum(1.0, u_rms / clip)
    return jnp.broadcast_to(k, (8, LANES))


def main_kernel(
    x_hbm, h_hbm, dg_hbm, du_hbm, do_hbm, wg_hbm, wu_hbm, wd_hbm,
    rg_hbm, cg_hbm, ru_hbm, cu_hbm, rd_hbm, cd_hbm, beta, rel, clip,
    gu, wu, wd, wg, rd_new, cd_new, rg_new, cg_new, ru_new, cu_new, kap, abc_u, bv_u,
    gd, gg, ring, xt, hs, ht, rowacc, abc_d, abc_g, cacc_d, cacc_g, cacc_u,
    bv_d, bv_g, rd, cd, rg, cg, ru, cu, rbuf_d, rbuf_g, rbuf_u, cbuf_d, cbuf_g, cbuf_u, sbuf, sacc, wacc,
    sem, r_send, r_recv, c_send, c_recv, s_send, s_recv,
):
    G, W = (gd, gg, gu), (wd, wg, wu)
    d_hbm, w_hbm = (do_hbm, dg_hbm, du_hbm), (wd_hbm, wg_hbm, wu_hbm)
    r_old, c_old = (rd, rg, ru), (cd, cg, cu)
    r_new, c_new = (rd_new, rg_new, ru_new), (cd_new, cg_new, cu_new)
    abc, cacc, bv = (abc_d, abc_g, abc_u), (cacc_d, cacc_g, cacc_u), (bv_d, bv_g, bv_u)
    rbuf, cbuf = (rbuf_d, rbuf_g, rbuf_u), (cbuf_d, cbuf_g, cbuf_u)
    _, me_c, me_r = place()

    def piece_copies(p):
        ks = slice(*PIECES[p])
        return (
            pltpu.make_async_copy(h_hbm.at[ks, :], hs.at[ks, :], sem.at[2 * p]),
            pltpu.make_async_copy(do_hbm.at[ks, :512], ring.at[0, ks, :512], sem.at[2 * p + 1]),
        )

    x_copy = pltpu.make_async_copy(x_hbm, ring.at[2, :, :512], sem.at[10])
    right_copy = pltpu.make_async_copy(do_hbm.at[:, 512:], ring.at[0, :, 512:], sem.at[11])

    places = (
        ring.at[1], hs.at[:, :1024], ring.at[2, :, :768],
        ring.at[0, :, :512], ring.at[1], ring.at[0, :, 512:1024], hs.at[:, :768],
    )

    def d_copy(j):
        mat, n0, n1 = BLOCKS[j]
        return pltpu.make_async_copy(d_hbm[mat].at[:, n0:n1], places[j], sem.at[(12, 13, 6, 7, 10, 8, 12)[j]])

    old_copies = [
        pltpu.make_async_copy(src, dst, sem.at[i])
        for i, (src, dst) in enumerate(zip((rd_hbm, cd_hbm, rg_hbm, cg_hbm, ru_hbm, cu_hbm), (rd, cd, rg, cg, ru, cu)))
    ]

    def w_copy(mat):
        return pltpu.make_async_copy(w_hbm[mat], W[mat], sem.at[(9, 11, 13)[mat]])

    late = slice(EARLY_COLS, SHAPES[UP][1] // LANES)
    COL_GROUPS = ((DOWN, slice(0, 8), 0), (GATE, slice(0, 22), 0), (UP, late, 0), (UP, slice(0, EARLY_COLS), 1))
    EARLY = 3

    def start_row(mat):
        row_copy(mat).start()

    def row_copy(mat):
        return remote(rbuf[mat].at[me_c], r_send.at[0], r_recv.at[mat], peer(1, 0))

    def start_cols(group):
        mat, part, send = COL_GROUPS[group]
        for d in (1, 2, 3):
            remote(cbuf[mat].at[me_r, part], c_send.at[send], c_recv.at[group], peer(0, d)).start()

    def all_cols(group):
        mat, part, send = COL_GROUPS[group]
        return remote(cbuf[mat].at[0:3, part], c_send.at[send], c_recv.at[group], peer(0, 1))

    def start_tiles(mat):
        me = me_c * ROWS + me_r
        for dc, dr in OTHERS:
            remote(sbuf.at[mat, me], s_send.at[0], s_recv.at[mat], peer(dc, dr)).start()

    def all_tiles(mat):
        return remote(sbuf.at[mat, 0:7], s_send.at[0], s_recv.at[mat], peer(0, 1))

    def start(copies):
        for c in copies:
            c.start()

    def wait(copies):
        for c in copies:
            c.wait()

    def stats_units(mat, n0, n1):
        units = []
        for r in range(0, SHAPES[mat][0], CHUNK):
            def unit(r=r):
                part = None
                for t in range(n0 // LANES, n1 // LANES):
                    g = G[mat][r:r + CHUNK, t * LANES:(t + 1) * LANES]
                    q = g * g
                    part = q if part is None else part + q
                    col = fold(q)
                    cols = pl.ds(t * LANES, LANES)
                    cacc[mat][:, cols] = col if r == 0 else cacc[mat][:, cols] + col
                rows = pl.ds(r, CHUNK)
                rowacc[rows, :] = part if n0 == 0 else rowacc[rows, :] + part
            units.append(unit)
        return units

    def row_units(mat):
        units = []
        for i in range(SHAPES[mat][0] // LANES):
            def rows(i=i):
                block = rowacc[i * LANES:(i + 1) * LANES, :].T
                rbuf[mat][me_c, i:i + 1, :] = jnp.sum(block, axis=0, keepdims=True)
            units.append(rows)
        return units

    def col_units(mat, t0, t1):
        units = []
        for t in range(t0, t1):
            def cols(t=t):
                cbuf[mat][me_r, t:t + 1, :] = jnp.sum(
                    cacc[mat][:, t * LANES:(t + 1) * LANES], axis=0, keepdims=True)
            units.append(cols)
        return units

    def sums_units(mat):
        return row_units(mat) + col_units(mat, 0, SHAPES[mat][1] // LANES)

    def w2_units(mat):
        units = []
        m, n = SHAPES[mat]
        for i in range(m // CHUNK):
            def unit(i=i):
                acc = None
                for t in range(n // LANES):
                    w = W[mat][i * CHUNK:(i + 1) * CHUNK, t * LANES:(t + 1) * LANES]
                    f = fold(w * w)
                    acc = f if acc is None else acc + f
                wacc[mat, i] = acc
            units.append(unit)
        return units

    def factor_units(mat):
        m, n = SHAPES[mat]
        mt, nt = TOTALS[mat]

        def new():
            b2 = beta[0]
            rows = rbuf[mat][0] + rbuf[mat][1]
            cols = (cbuf[mat][0] + cbuf[mat][1]) + (cbuf[mat][2] + cbuf[mat][3])
            rn = b2 * r_old[mat][...] + (1.0 - b2) * (rows * (1.0 / nt) + EPS_SQ)
            cn = b2 * c_old[mat][...] + (1.0 - b2) * (cols * (1.0 / mt) + EPS_SQ)
            r_new[mat][...] = rn
            c_new[mat][...] = cn
            bv[mat][...] = lax.rsqrt(cn)

        units = [new]
        for i in range(m // LANES):
            def unit(i=i):
                a = lax.rsqrt(r_new[mat][i:i + 1, :])
                abc[mat][i * LANES:(i + 1) * LANES, :] = jnp.broadcast_to(a, (LANES, LANES)).T
            units.append(unit)
        return units

    def scale_units(mat):
        units = []
        m, n = SHAPES[mat]
        for i in range(m // CHUNK):
            def unit(i=i):
                acc = None
                rows = slice(i * CHUNK, (i + 1) * CHUNK)
                a = abc[mat][rows, :]
                for t in range(n // LANES):
                    h = G[mat][rows, t * LANES:(t + 1) * LANES] * a * bv[mat][t:t + 1, :]
                    f = fold(h * h)
                    acc = f if acc is None else acc + f
                sacc[mat, i] = acc
            units.append(unit)
        return units

    def update_units(mat):
        def step():
            kap[mat] = step_of(mat, sbuf.at[mat], rel[0], clip[0])

        units = [step]
        m, n = SHAPES[mat]
        for r in range(0, m, CHUNK):
            def unit(r=r):
                ka = abc[mat][r:r + CHUNK, :] * kap[mat, 0:1, :]
                for t in range(n // LANES):
                    cols = slice(t * LANES, (t + 1) * LANES)
                    W[mat][r:r + CHUNK, cols] = (
                        W[mat][r:r + CHUNK, cols] - G[mat][r:r + CHUNK, cols] * ka * bv[mat][t:t + 1, :])
            units.append(unit)
        return units

    def tile_unit(mat):
        def unit():
            _, c, r = place()
            chunks = SHAPES[mat][0] // CHUNK
            sbuf[mat, c * ROWS + r] = scalar_tile(
                jnp.sum(sacc[mat, :chunks], axis=0), jnp.sum(wacc[mat, :chunks], axis=0), r_new[mat][...])
        return [unit]

    def h_units(p):
        k0, k1 = PIECES[p]
        units = []
        for k in range(k0, k1, 256):
            for i in range(0, SHAPES[DOWN][0], LANES):
                def unit(k=k, i=i):
                    ht[i:i + LANES, k:k + 256] = hs[k:k + 256, i:i + LANES].T
                units.append(unit)
        return units

    def x_units():
        units = []
        for k in range(0, K, 256):
            for i in range(0, 512, LANES):
                def unit(k=k, i=i):
                    xt[i:i + LANES, k:k + 256] = ring[2, k:k + 256, i:i + LANES].T
                units.append(unit)
        return units

    def down_dots(p):
        ks = slice(*PIECES[p])
        out = []
        for r in range(0, 1408, 352):
            def dot(r=r):
                rs = slice(r, r + 352)
                part = jnp.dot(ht[rs, ks], ring[0, ks, :512], preferred_element_type=F32)
                gd[rs, :512] = part if p == 0 else gd[rs, :512] + part
            out.append(dot)
        return out

    def right_dots():
        out = []
        for r in range(0, 1408, 352):
            def dot(r=r):
                rs = slice(r, r + 352)
                gd[rs, 512:] = jnp.dot(ht[rs, :], ring[0, :, 512:], preferred_element_type=F32)
            out.append(dot)
        return out

    def dots_of(j):
        mat, n0, n1 = BLOCKS[j]
        out = []

        def dot(r0, r1, c0, c1):
            def run():
                G[mat][r0:r1, n0 + c0:n0 + c1] = jnp.dot(
                    xt[r0:r1, :], places[j][:, c0:c1], preferred_element_type=F32)
            return run

        w = n1 - n0
        for c in range(0, w, 512):
            if c + 512 <= w:
                out.append(dot(0, 512, c, c + 512))
            else:
                out += [dot(0, 256, c, w), dot(256, 512, c, w)]
        return out

    def run(units):
        for unit in units:
            unit()

    for p in (0, 1, 2):
        start(piece_copies(p))
    barrier = pltpu.get_barrier_semaphore()
    signal_entry(barrier)
    wait(piece_copies(0))
    start(piece_copies(3))
    start(piece_copies(4))
    right_copy.start()
    x_copy.start()
    run(h_units(0))
    for p in range(4):
        wait(piece_copies(p + 1))
        if p == 1:
            d_copy(0).start()
        interleave(down_dots(p), h_units(p + 1))
    d_copy(1).start()
    interleave(down_dots(4), [])
    start(old_copies)
    right_copy.wait()
    x_copy.wait()
    interleave(right_dots(), x_units() + stats_units(DOWN, 0, 512))
    d_copy(2).start()
    d_copy(3).start()
    d_copy(5).start()
    w_copy(DOWN).start()

    d_copy(0).wait()
    wait(old_copies)
    interleave(dots_of(0), stats_units(DOWN, 512, 1024) + sums_units(DOWN))
    pl.semaphore_wait(barrier, len(OTHERS))
    start_row(DOWN)
    start_cols(DOWN)
    d_copy(4).start()
    w_copy(GATE).start()

    d_copy(1).wait()
    d_copy(2).wait()
    interleave(dots_of(1), stats_units(GATE, 0, 1024))
    interleave(dots_of(2), stats_units(GATE, 1024, 2048))
    d_copy(6).start()
    w_copy(UP).start()

    d_copy(3).wait()
    interleave(dots_of(3), stats_units(GATE, 2048, 2816) + sums_units(GATE))
    row_copy(DOWN).wait_send()
    all_cols(DOWN).wait_send()
    start_row(GATE)
    start_cols(GATE)

    d_copy(4).wait()
    d_copy(5).wait()
    row_copy(DOWN).wait_recv()
    all_cols(DOWN).wait_recv()
    interleave(dots_of(4), factor_units(DOWN) + scale_units(DOWN))
    interleave(dots_of(5), stats_units(UP, 0, 512) + stats_units(UP, 512, 1536))

    d_copy(6).wait()
    w_copy(DOWN).wait()
    interleave(
        dots_of(6),
        w2_units(DOWN) + tile_unit(DOWN) + stats_units(UP, 1536, 2048) + col_units(UP, 0, EARLY_COLS))
    start_cols(EARLY)
    start_tiles(DOWN)

    run(stats_units(UP, 2048, 2816) + row_units(UP) + col_units(UP, EARLY_COLS, 22))
    row_copy(GATE).wait_send()
    all_cols(GATE).wait_send()
    start_row(UP)
    start_cols(UP)
    w_copy(GATE).wait()
    w_copy(UP).wait()
    row_copy(GATE).wait_recv()
    all_cols(GATE).wait_recv()
    run(factor_units(GATE) + scale_units(GATE) + w2_units(GATE) + tile_unit(GATE))
    all_tiles(DOWN).wait_send()
    start_tiles(GATE)
    run(w2_units(UP))
    all_cols(EARLY).wait_recv()
    row_copy(UP).wait_recv()
    all_cols(UP).wait_recv()
    run(factor_units(UP) + scale_units(UP) + tile_unit(UP))
    all_tiles(GATE).wait_send()
    start_tiles(UP)
    all_tiles(DOWN).wait_recv()
    run(update_units(DOWN))
    all_tiles(GATE).wait_recv()
    run(update_units(GATE))
    row_copy(UP).wait_send()
    all_cols(UP).wait_send()
    all_cols(EARLY).wait_send()
    all_tiles(UP).wait_send()
    all_tiles(UP).wait_recv()
    kap[UP] = step_of(UP, sbuf.at[UP], rel[0], clip[0])


def update_kernel(
    gu, wu, wd, wg, rd, cd, rg, cg, ru, cu, kap, abc, bv,
    wu_o, wd_o, wg_o, rd_o, cd_o, rg_o, cg_o, ru_o, cu_o, stage, sem,
):
    srcs = (wd, wg, rd, cd, rg, cg, ru, cu)
    dsts = (wd_o, wg_o, rd_o, cd_o, rg_o, cg_o, ru_o, cu_o)
    copies = [pltpu.make_async_copy(src, dst, sem) for src, dst in zip(srcs, dsts)]
    for c in copies:
        c.start()
    m, n = SHAPES[UP]
    k = kap[UP, 0:1, :]
    for r in range(0, m, CHUNK):
        ka = abc[r:r + CHUNK, :] * k
        for t in range(n // LANES):
            cols = slice(t * LANES, (t + 1) * LANES)
            stage[r:r + CHUNK, cols] = wu[r:r + CHUNK, cols] - gu[r:r + CHUNK, cols] * ka * bv[t:t + 1, :]
        copies.append(pltpu.make_async_copy(stage.at[r:r + CHUNK, :], wu_o.at[r:r + CHUNK, :], sem))
        copies[-1].start()
    for copy in copies:
        copy.wait()


VMEM_LIMIT = 41 * 1024 * 1024


def local_program(x_in, h_act, d_gate, d_up, d_out, w_gate, w_up, w_down, r_gate, c_gate, r_up, c_up, r_down, c_down, beta_two, rel_step, clip_thr):
    any_spec = pl.BlockSpec(memory_space=pl.ANY)
    vmem_spec = pl.BlockSpec(memory_space=pltpu.VMEM)
    smem_spec = pl.BlockSpec(memory_space=pltpu.SMEM)

    def stat_shape(v):
        return (v // LANES, LANES)

    stats = [v.reshape(stat_shape(v.shape[0])) for v in (r_gate, c_gate, r_up, c_up, r_down, c_down)]
    beta, rel, clip = [v.reshape(1) for v in (beta_two, rel_step, clip_thr)]
    rows = [stat_shape(m) for m, n in SHAPES]
    cols = [stat_shape(n) for m, n in SHAPES]
    dma = pltpu.SemaphoreType.DMA

    stat_pairs = [s for pair in zip(rows, cols) for s in pair]
    outs = pl.pallas_call(
        main_kernel,
        out_shape=[pltpu.VMEM(SHAPES[UP], F32)] * 2 + [pltpu.VMEM(s, F32) for s in SHAPES[:2]]
        + [pltpu.VMEM(s, F32) for s in stat_pairs]
        + [pltpu.VMEM((3, 8, LANES), F32), pltpu.VMEM((512, LANES), F32), pltpu.VMEM(cols[UP], F32)],
        in_specs=[any_spec] * 14 + [smem_spec] * 3,
        out_specs=[vmem_spec] * 13,
        scratch_shapes=[
            pltpu.VMEM(SHAPES[DOWN], F32),
            pltpu.VMEM(SHAPES[GATE], F32),
            pltpu.VMEM((3, K, 1024), BF16),
            pltpu.VMEM((512, K), BF16),
            pltpu.VMEM((K, 1408), BF16),
            pltpu.VMEM((1408, K), BF16),
            pltpu.VMEM((1408, LANES), F32),
            pltpu.VMEM((1408, LANES), F32),
            pltpu.VMEM((512, LANES), F32),
        ]
        + [pltpu.VMEM((8, n), F32) for m, n in SHAPES]
        + [pltpu.VMEM(s, F32) for s in cols[:2]]
        + [pltpu.VMEM(s, F32) for s in stat_pairs]
        + [pltpu.VMEM((COLS, *s), F32) for s in rows]
        + [pltpu.VMEM((ROWS, *s), F32) for s in cols]
        + [
            pltpu.VMEM((3, ROWS * COLS, 4, LANES), F32),
            pltpu.VMEM((3, 22, 8, LANES), F32),
            pltpu.VMEM((3, 22, 8, LANES), F32),
            dma((14,)), dma((1,)), dma((3,)), dma((2,)), dma((4,)), dma((1,)), dma((3,)),
        ],
        compiler_params=pltpu.CompilerParams(
            collective_id=0, has_side_effects=True, vmem_limit_bytes=VMEM_LIMIT),
        name="main",
    )(
        *[pltpu.with_memory_space_constraint(v, pltpu.HBM)
          for v in (x_in, h_act, d_gate, d_up, d_out, w_gate, w_up, w_down, *stats)],
        beta, rel, clip)
    held = [pltpu.with_memory_space_constraint(v, pltpu.VMEM) for v in outs]
    res = pl.pallas_call(
        update_kernel,
        out_shape=[jax.ShapeDtypeStruct(s, F32) for s in (SHAPES[UP], *SHAPES[:2], *stat_pairs)],
        in_specs=[vmem_spec] * 13,
        out_specs=[any_spec] * 9,
        scratch_shapes=[pltpu.VMEM(SHAPES[UP], F32), dma],
        compiler_params=pltpu.CompilerParams(vmem_limit_bytes=VMEM_LIMIT),
        name="update",
    )(*held)
    up, down, gate, rd_n, cd_n, rg_n, cg_n, ru_n, cu_n = res
    flat = [v.reshape(-1) for v in (rg_n, cg_n, ru_n, cu_n, rd_n, cd_n)]
    return (gate, up, down, *flat)


def solution(mesh):
    act_spec = P(None, "row")
    cot_spec = P(None, "col")
    w_spec = P("row", "col")
    r_spec = P("row")
    c_spec = P("col")
    s_spec = P()
    return jax.shard_map(local_program, mesh=mesh, in_specs=(act_spec, act_spec, cot_spec, cot_spec, cot_spec, w_spec, w_spec, w_spec, r_spec, c_spec, r_spec, c_spec, r_spec, c_spec, s_spec, s_spec, s_spec), out_specs=(w_spec, w_spec, w_spec, r_spec, c_spec, r_spec, c_spec, r_spec, c_spec), check_vma=False)
```

```python
import jax
import jax.numpy as jnp
from jax import lax
from jax.experimental import pallas as pl
from jax.experimental.pallas import tpu as pltpu
from jax.sharding import PartitionSpec as P

EPS_SQ = 1e-30
EPS_SCALE = 1e-3
LANES = 128
K = 2048
ROWS, COLS = 4, 2
F32 = jnp.float32
BF16 = jnp.bfloat16
MESH = pl.DeviceIdType.MESH

DOWN, GATE, UP = 0, 1, 2
SHAPES = ((1408, 1024), (512, 2816), (512, 2816))
TOTALS = tuple((m * ROWS, n * COLS) for m, n in SHAPES)
PIECES = ((0, 256), (256, 512), (512, 1024), (1024, 1536), (1536, 2048))
GATE_BLOCKS = ((0, 1024), (1024, 2048), (2048, 2816))
UP_BLOCKS = ((0, 512), (512, 1536), (1536, 2048), (2048, 2816))
BLOCKS = tuple((GATE, *b) for b in GATE_BLOCKS) + tuple((UP, *b) for b in UP_BLOCKS)
EARLY_COLS = 16
CHUNK = 64
OTHERS = [(dc, dr) for dc in range(COLS) for dr in range(ROWS) if (dc, dr) != (0, 0)]


def interleave(dots, units):
    done = 0
    for i, dot in enumerate(dots):
        upto = len(units) * (i + 1) // len(dots)
        for unit in units[done:upto]:
            unit()
        done = upto
        dot()


def fold(x):
    return jnp.sum(x.reshape(x.shape[0] // 8, 8, x.shape[1]), axis=0)


def place():
    return lax.axis_index("data"), lax.axis_index("col"), lax.axis_index("row")


def peer(dc, dr):
    d, c, r = place()
    return (d, lax.rem(c + dc, COLS), lax.rem(r + dr, ROWS))


def signal_entry(barrier):
    for dc, dr in OTHERS:
        pl.semaphore_signal(barrier, inc=1, device_id=peer(dc, dr), device_id_type=MESH)


def remote(ref, send, recv, to):
    return pltpu.make_async_remote_copy(
        src_ref=ref, dst_ref=ref, send_sem=send, recv_sem=recv, device_id=to, device_id_type=MESH)


def scalar_tile(s, w, r):
    rows = [jnp.sum(v, axis=0, keepdims=True) for v in (s, w, r)]
    return jnp.concatenate(rows + [jnp.zeros((1, LANES), F32)], axis=0)


def sums_of(buf):
    tot = buf[0]
    for i in range(1, ROWS * COLS):
        tot = tot + buf[i]
    return jnp.broadcast_to(jnp.sum(tot, axis=1, keepdims=True), tot.shape)


def step_of(mat, tot, rel, clip):
    mt, nt = TOTALS[mat]
    s, w, r = tot[0:1, :], tot[1:2, :], tot[2:3, :]
    r_mean = r * (1.0 / (COLS * mt))
    u_rms = jnp.sqrt(s * (1.0 / (mt * nt)) * r_mean)
    w_rms = jnp.sqrt(w * (1.0 / (mt * nt)))
    step = rel * jnp.maximum(EPS_SCALE, w_rms)
    return step * jnp.sqrt(r_mean) / jnp.maximum(1.0, u_rms / clip)


def main_kernel(
    x_hbm, h_hbm, dg_hbm, du_hbm, do_hbm, wg_hbm, wu_hbm, wd_hbm,
    rg_hbm, cg_hbm, ru_hbm, cu_hbm, rd_hbm, cd_hbm, beta,
    gd, gg, gu, wd, wg, wu, rd_new, cd_new, rg_new, cg_new, ru_new, cu_new, sums,
    abc_d, abc_g, abc_u, bv_d, bv_g, bv_u,
    ring, xt, hs, ht, rowacc, cacc_d, cacc_g, cacc_u,
    rd, cd, rg, cg, ru, cu, rbuf_d, rbuf_g, rbuf_u, cbuf_d, cbuf_g, cbuf_u, sbuf, sacc, wacc,
    sem, r_send, r_recv, c_send, c_recv, s_send, s_recv,
):
    G, W = (gd, gg, gu), (wd, wg, wu)
    d_hbm, w_hbm = (do_hbm, dg_hbm, du_hbm), (wd_hbm, wg_hbm, wu_hbm)
    r_old, c_old = (rd, rg, ru), (cd, cg, cu)
    r_new, c_new = (rd_new, rg_new, ru_new), (cd_new, cg_new, cu_new)
    abc, cacc, bv = (abc_d, abc_g, abc_u), (cacc_d, cacc_g, cacc_u), (bv_d, bv_g, bv_u)
    rbuf, cbuf = (rbuf_d, rbuf_g, rbuf_u), (cbuf_d, cbuf_g, cbuf_u)
    _, me_c, me_r = place()

    def piece_copies(p):
        ks = slice(*PIECES[p])
        return (
            pltpu.make_async_copy(h_hbm.at[ks, :], hs.at[ks, :], sem.at[2 * p]),
            pltpu.make_async_copy(do_hbm.at[ks, :512], ring.at[0, ks, :512], sem.at[2 * p + 1]),
        )

    x_copy = pltpu.make_async_copy(x_hbm, ring.at[2, :, :512], sem.at[10])
    right_copy = pltpu.make_async_copy(do_hbm.at[:, 512:], ring.at[0, :, 512:], sem.at[11])

    places = (
        ring.at[1], hs.at[:, :1024], ring.at[2, :, :768],
        ring.at[0, :, :512], ring.at[1], ring.at[0, :, 512:1024], hs.at[:, :768],
    )

    def d_copy(j):
        mat, n0, n1 = BLOCKS[j]
        return pltpu.make_async_copy(d_hbm[mat].at[:, n0:n1], places[j], sem.at[(12, 13, 6, 7, 10, 8, 12)[j]])

    old_copies = [
        pltpu.make_async_copy(src, dst, sem.at[i])
        for i, (src, dst) in enumerate(zip((rd_hbm, cd_hbm, rg_hbm, cg_hbm, ru_hbm, cu_hbm), (rd, cd, rg, cg, ru, cu)))
    ]

    def w_copy(mat):
        return pltpu.make_async_copy(w_hbm[mat], W[mat], sem.at[(9, 11, 13)[mat]])

    late = slice(EARLY_COLS, SHAPES[UP][1] // LANES)
    COL_GROUPS = ((DOWN, slice(0, 8), 0), (GATE, slice(0, 22), 0), (UP, late, 0), (UP, slice(0, EARLY_COLS), 1))
    EARLY = 3

    def start_row(mat):
        row_copy(mat).start()

    def row_copy(mat):
        return remote(rbuf[mat].at[me_c], r_send.at[0], r_recv.at[mat], peer(1, 0))

    def start_cols(group):
        mat, part, send = COL_GROUPS[group]
        for d in (1, 2, 3):
            remote(cbuf[mat].at[me_r, part], c_send.at[send], c_recv.at[group], peer(0, d)).start()

    def all_cols(group):
        mat, part, send = COL_GROUPS[group]
        return remote(cbuf[mat].at[0:3, part], c_send.at[send], c_recv.at[group], peer(0, 1))

    def start_tiles(mat):
        me = me_c * ROWS + me_r
        for dc, dr in OTHERS:
            remote(sbuf.at[mat, me], s_send.at[0], s_recv.at[mat], peer(dc, dr)).start()

    def all_tiles(mat):
        return remote(sbuf.at[mat, 0:7], s_send.at[0], s_recv.at[mat], peer(0, 1))

    def start(copies):
        for c in copies:
            c.start()

    def wait(copies):
        for c in copies:
            c.wait()

    def stats_units(mat, n0, n1):
        units = []
        for r in range(0, SHAPES[mat][0], CHUNK):
            def unit(r=r):
                part = None
                for t in range(n0 // LANES, n1 // LANES):
                    g = G[mat][r:r + CHUNK, t * LANES:(t + 1) * LANES]
                    q = g * g
                    part = q if part is None else part + q
                    col = fold(q)
                    cols = pl.ds(t * LANES, LANES)
                    cacc[mat][:, cols] = col if r == 0 else cacc[mat][:, cols] + col
                rows = pl.ds(r, CHUNK)
                rowacc[rows, :] = part if n0 == 0 else rowacc[rows, :] + part
            units.append(unit)
        return units

    def row_units(mat):
        units = []
        for i in range(SHAPES[mat][0] // LANES):
            def rows(i=i):
                block = rowacc[i * LANES:(i + 1) * LANES, :].T
                rbuf[mat][me_c, i:i + 1, :] = jnp.sum(block, axis=0, keepdims=True)
            units.append(rows)
        return units

    def col_units(mat, t0, t1):
        units = []
        for t in range(t0, t1):
            def cols(t=t):
                cbuf[mat][me_r, t:t + 1, :] = jnp.sum(
                    cacc[mat][:, t * LANES:(t + 1) * LANES], axis=0, keepdims=True)
            units.append(cols)
        return units

    def sums_units(mat):
        return row_units(mat) + col_units(mat, 0, SHAPES[mat][1] // LANES)

    def w2_units(mat):
        units = []
        m, n = SHAPES[mat]
        for i in range(m // CHUNK):
            def unit(i=i):
                acc = None
                for t in range(n // LANES):
                    w = W[mat][i * CHUNK:(i + 1) * CHUNK, t * LANES:(t + 1) * LANES]
                    f = fold(w * w)
                    acc = f if acc is None else acc + f
                wacc[mat, i] = acc
            units.append(unit)
        return units

    def factor_units(mat):
        m, n = SHAPES[mat]
        mt, nt = TOTALS[mat]

        def new():
            b2 = beta[0]
            rows = rbuf[mat][0] + rbuf[mat][1]
            cols = (cbuf[mat][0] + cbuf[mat][1]) + (cbuf[mat][2] + cbuf[mat][3])
            rn = b2 * r_old[mat][...] + (1.0 - b2) * (rows * (1.0 / nt) + EPS_SQ)
            cn = b2 * c_old[mat][...] + (1.0 - b2) * (cols * (1.0 / mt) + EPS_SQ)
            r_new[mat][...] = rn
            c_new[mat][...] = cn
            bv[mat][...] = lax.rsqrt(cn)

        units = [new]
        for i in range(m // LANES):
            def unit(i=i):
                a = lax.rsqrt(r_new[mat][i:i + 1, :])
                abc[mat][i * LANES:(i + 1) * LANES, :] = jnp.broadcast_to(a, (LANES, LANES)).T
            units.append(unit)
        return units

    def scale_units(mat):
        units = []
        m, n = SHAPES[mat]
        for i in range(m // CHUNK):
            def unit(i=i):
                acc = None
                rows = slice(i * CHUNK, (i + 1) * CHUNK)
                for t in range(n // LANES):
                    h = G[mat][rows, t * LANES:(t + 1) * LANES] * bv[mat][t:t + 1, :]
                    acc = h * h if acc is None else acc + h * h
                a = abc[mat][rows, :]
                sacc[mat, i] = fold(acc * (a * a))
            units.append(unit)
        return units

    def tile_unit(mat):
        def unit():
            _, c, r = place()
            chunks = SHAPES[mat][0] // CHUNK
            sbuf[mat, c * ROWS + r] = scalar_tile(
                jnp.sum(sacc[mat, :chunks], axis=0), jnp.sum(wacc[mat, :chunks], axis=0), r_new[mat][...])
        return [unit]

    def h_units(p):
        k0, k1 = PIECES[p]
        units = []
        for k in range(k0, k1, 256):
            for i in range(0, SHAPES[DOWN][0], LANES):
                def unit(k=k, i=i):
                    ht[i:i + LANES, k:k + 256] = hs[k:k + 256, i:i + LANES].T
                units.append(unit)
        return units

    def x_units():
        units = []
        for k in range(0, K, 256):
            for i in range(0, 512, LANES):
                def unit(k=k, i=i):
                    xt[i:i + LANES, k:k + 256] = ring[2, k:k + 256, i:i + LANES].T
                units.append(unit)
        return units

    def down_dots(p):
        ks = slice(*PIECES[p])
        out = []
        for r in range(0, 1408, 352):
            def dot(r=r):
                rs = slice(r, r + 352)
                part = jnp.dot(ht[rs, ks], ring[0, ks, :512], preferred_element_type=F32)
                gd[rs, :512] = part if p == 0 else gd[rs, :512] + part
            out.append(dot)
        return out

    def right_dots():
        out = []
        for r in range(0, 1408, 352):
            def dot(r=r):
                rs = slice(r, r + 352)
                gd[rs, 512:] = jnp.dot(ht[rs, :], ring[0, :, 512:], preferred_element_type=F32)
            out.append(dot)
        return out

    def dots_of(j):
        mat, n0, n1 = BLOCKS[j]
        out = []

        def dot(r0, r1, c0, c1):
            def run():
                G[mat][r0:r1, n0 + c0:n0 + c1] = jnp.dot(
                    xt[r0:r1, :], places[j][:, c0:c1], preferred_element_type=F32)
            return run

        w = n1 - n0
        for c in range(0, w, 512):
            if c + 512 <= w:
                out.append(dot(0, 512, c, c + 512))
            else:
                out += [dot(0, 256, c, w), dot(256, 512, c, w)]
        return out

    def run(units):
        for unit in units:
            unit()

    for p in (0, 1, 2):
        start(piece_copies(p))
    barrier = pltpu.get_barrier_semaphore()
    signal_entry(barrier)
    wait(piece_copies(0))
    start(piece_copies(3))
    start(piece_copies(4))
    right_copy.start()
    x_copy.start()
    run(h_units(0))
    for p in range(4):
        wait(piece_copies(p + 1))
        if p == 1:
            d_copy(0).start()
        interleave(down_dots(p), h_units(p + 1))
    d_copy(1).start()
    interleave(down_dots(4), [])
    start(old_copies)
    right_copy.wait()
    x_copy.wait()
    interleave(right_dots(), x_units() + stats_units(DOWN, 0, 512))
    d_copy(2).start()
    d_copy(3).start()
    d_copy(5).start()
    w_copy(DOWN).start()

    d_copy(0).wait()
    wait(old_copies)
    interleave(dots_of(0), stats_units(DOWN, 512, 1024) + sums_units(DOWN))
    pl.semaphore_wait(barrier, len(OTHERS))
    start_row(DOWN)
    start_cols(DOWN)
    d_copy(4).start()
    w_copy(GATE).start()

    d_copy(1).wait()
    d_copy(2).wait()
    interleave(dots_of(1), stats_units(GATE, 0, 1024))
    interleave(dots_of(2), stats_units(GATE, 1024, 2048))
    d_copy(6).start()
    w_copy(UP).start()

    d_copy(3).wait()
    interleave(dots_of(3), stats_units(GATE, 2048, 2816) + sums_units(GATE))
    row_copy(DOWN).wait_send()
    all_cols(DOWN).wait_send()
    start_row(GATE)
    start_cols(GATE)

    d_copy(4).wait()
    d_copy(5).wait()
    row_copy(DOWN).wait_recv()
    all_cols(DOWN).wait_recv()
    interleave(dots_of(4), factor_units(DOWN) + scale_units(DOWN))
    interleave(dots_of(5), stats_units(UP, 0, 512) + stats_units(UP, 512, 1536))

    d_copy(6).wait()
    w_copy(DOWN).wait()
    interleave(
        dots_of(6),
        w2_units(DOWN) + tile_unit(DOWN) + stats_units(UP, 1536, 2048) + col_units(UP, 0, EARLY_COLS))
    start_cols(EARLY)
    start_tiles(DOWN)

    run(stats_units(UP, 2048, 2816) + row_units(UP) + col_units(UP, EARLY_COLS, 22))
    row_copy(GATE).wait_send()
    all_cols(GATE).wait_send()
    start_row(UP)
    start_cols(UP)
    w_copy(GATE).wait()
    w_copy(UP).wait()
    row_copy(GATE).wait_recv()
    all_cols(GATE).wait_recv()
    run(factor_units(GATE) + scale_units(GATE) + w2_units(GATE) + tile_unit(GATE))
    all_tiles(DOWN).wait_send()
    start_tiles(GATE)
    run(w2_units(UP))
    all_cols(EARLY).wait_recv()
    row_copy(UP).wait_recv()
    all_cols(UP).wait_recv()
    run(factor_units(UP) + scale_units(UP) + tile_unit(UP))
    all_tiles(GATE).wait_send()
    start_tiles(UP)
    all_tiles(DOWN).wait_recv()
    sums[DOWN] = sums_of(sbuf.at[DOWN])
    all_tiles(GATE).wait_recv()
    sums[GATE] = sums_of(sbuf.at[GATE])
    row_copy(UP).wait_send()
    all_cols(UP).wait_send()
    all_cols(EARLY).wait_send()
    all_tiles(UP).wait_send()
    all_tiles(UP).wait_recv()
    sums[UP] = sums_of(sbuf.at[UP])


def update_kernel(
    gd, gg, gu, wd, wg, wu, rd, cd, rg, cg, ru, cu, sums, abc_d, abc_g, abc_u, bv_d, bv_g, bv_u, rel, clip,
    wd_o, wg_o, wu_o, rd_o, cd_o, rg_o, cg_o, ru_o, cu_o, stage_d, stage_g, stage_u, sem,
):
    copies = []

    def write(src, dst):
        copies.append(pltpu.make_async_copy(src, dst, sem))
        copies[-1].start()

    steps = [step_of(mat, sums[mat], rel[...], clip[...]) for mat in range(3)]
    for mat, (g, w, abc, bv, stage, out) in enumerate((
        (gd, wd, abc_d, bv_d, stage_d, wd_o), (gg, wg, abc_g, bv_g, stage_g, wg_o), (gu, wu, abc_u, bv_u, stage_u, wu_o),
    )):
        m, n = SHAPES[mat]
        for r in range(0, m, CHUNK):
            rows = slice(r, r + CHUNK)
            ka = abc[rows, :] * steps[mat]
            for t in range(n // LANES):
                cols = slice(t * LANES, (t + 1) * LANES)
                stage[rows, cols] = w[rows, cols] - g[rows, cols] * ka * bv[t:t + 1, :]
            write(stage.at[rows, :], out.at[rows, :])
        if mat == DOWN:
            for src, dst in ((rd, rd_o), (cd, cd_o), (rg, rg_o), (cg, cg_o), (ru, ru_o), (cu, cu_o)):
                write(src, dst)
    for copy in copies:
        copy.wait()


VMEM_LIMIT = 30880000


def local_program(x_in, h_act, d_gate, d_up, d_out, w_gate, w_up, w_down, r_gate, c_gate, r_up, c_up, r_down, c_down, beta_two, rel_step, clip_thr):
    any_spec = pl.BlockSpec(memory_space=pl.ANY)
    vmem_spec = pl.BlockSpec(memory_space=pltpu.VMEM)
    smem_spec = pl.BlockSpec(memory_space=pltpu.SMEM)

    def stat_shape(v):
        return (v // LANES, LANES)

    stats = [v.reshape(stat_shape(v.shape[0])) for v in (r_gate, c_gate, r_up, c_up, r_down, c_down)]
    beta = beta_two.reshape(1)
    rel, clip = [lax.ppermute(v.reshape(1, 1), "data", [(0, 1), (1, 0)]) for v in (rel_step, clip_thr)]
    rows = [stat_shape(m) for m, n in SHAPES]
    cols = [stat_shape(n) for m, n in SHAPES]
    dma = pltpu.SemaphoreType.DMA

    stat_pairs = [s for pair in zip(rows, cols) for s in pair]
    outs = pl.pallas_call(
        main_kernel,
        out_shape=[pltpu.VMEM(s, F32) for s in (*SHAPES, *SHAPES, *stat_pairs, (3, 4, LANES))]
        + [pltpu.VMEM((m, LANES), F32) for m, n in SHAPES] + [pltpu.VMEM(s, F32) for s in cols],
        in_specs=[any_spec] * 14 + [smem_spec],
        out_specs=[vmem_spec] * 19,
        scratch_shapes=[
            pltpu.VMEM((3, K, 1024), BF16),
            pltpu.VMEM((512, K), BF16),
            pltpu.VMEM((K, 1408), BF16),
            pltpu.VMEM((1408, K), BF16),
            pltpu.VMEM((1408, LANES), F32),
        ]
        + [pltpu.VMEM((8, n), F32) for m, n in SHAPES]
        + [pltpu.VMEM(s, F32) for s in stat_pairs]
        + [pltpu.VMEM((COLS, *s), F32) for s in rows]
        + [pltpu.VMEM((ROWS, *s), F32) for s in cols]
        + [
            pltpu.VMEM((3, ROWS * COLS, 4, LANES), F32),
            pltpu.VMEM((3, 22, 8, LANES), F32),
            pltpu.VMEM((3, 22, 8, LANES), F32),
            dma((14,)), dma((1,)), dma((3,)), dma((2,)), dma((4,)), dma((1,)), dma((3,)),
        ],
        compiler_params=pltpu.CompilerParams(
            collective_id=0, has_side_effects=True, vmem_limit_bytes=VMEM_LIMIT),
        name="main",
    )(
        *[pltpu.with_memory_space_constraint(v, pltpu.HBM)
          for v in (x_in, h_act, d_gate, d_up, d_out, w_gate, w_up, w_down, *stats)],
        beta)
    held = [pltpu.with_memory_space_constraint(v, pltpu.VMEM) for v in (*outs, rel, clip)]
    res = pl.pallas_call(
        update_kernel,
        out_shape=[jax.ShapeDtypeStruct(s, F32) for s in (*SHAPES, *stat_pairs)],
        in_specs=[vmem_spec] * 21,
        out_specs=[any_spec] * 9,
        scratch_shapes=[pltpu.VMEM(s, F32) for s in SHAPES] + [dma],
        compiler_params=pltpu.CompilerParams(vmem_limit_bytes=VMEM_LIMIT),
        name="update",
    )(*held)
    down, gate, up, rd_n, cd_n, rg_n, cg_n, ru_n, cu_n = res
    flat = [v.reshape(-1) for v in (rg_n, cg_n, ru_n, cu_n, rd_n, cd_n)]
    return (gate, up, down, *flat)


def solution(mesh):
    act_spec = P(None, "row")
    cot_spec = P(None, "col")
    w_spec = P("row", "col")
    r_spec = P("row")
    c_spec = P("col")
    s_spec = P()
    return jax.shard_map(local_program, mesh=mesh, in_specs=(act_spec, act_spec, cot_spec, cot_spec, cot_spec, w_spec, w_spec, w_spec, r_spec, c_spec, r_spec, c_spec, r_spec, c_spec, s_spec, s_spec, s_spec), out_specs=(w_spec, w_spec, w_spec, r_spec, c_spec, r_spec, c_spec, r_spec, c_spec), check_vma=False)
```

```python
import jax
import jax.numpy as jnp
from jax import lax
from jax.experimental import pallas as pl
from jax.experimental.pallas import tpu as pltpu
from jax.sharding import PartitionSpec as P

EPS_SQ = 1e-30
EPS_SCALE = 1e-3
LANES = 128
K = 2048
ROWS, COLS = 4, 2
F32 = jnp.float32
BF16 = jnp.bfloat16
MESH = pl.DeviceIdType.MESH

DOWN, GATE, UP = 0, 1, 2
SHAPES = ((1408, 1024), (512, 2816), (512, 2816))
TOTALS = tuple((m * ROWS, n * COLS) for m, n in SHAPES)
PIECES = ((0, 256), (256, 512), (512, 1024), (1024, 1536), (1536, 2048))
GATE_BLOCKS = ((0, 1024), (1024, 2048), (2048, 2816))
UP_BLOCKS = ((0, 512), (512, 1536), (1536, 2048), (2048, 2816))
BLOCKS = tuple((GATE, *b) for b in GATE_BLOCKS) + tuple((UP, *b) for b in UP_BLOCKS)
EARLY_COLS = 16
CHUNK = 64
OTHERS = [(dc, dr) for dc in range(COLS) for dr in range(ROWS) if (dc, dr) != (0, 0)]


def interleave(dots, units):
    done = 0
    for i, dot in enumerate(dots):
        upto = len(units) * (i + 1) // len(dots)
        for unit in units[done:upto]:
            unit()
        done = upto
        dot()


def fold(x):
    return jnp.sum(x.reshape(x.shape[0] // 8, 8, x.shape[1]), axis=0)


def place():
    return lax.axis_index("data"), lax.axis_index("col"), lax.axis_index("row")


def peer(dc, dr):
    d, c, r = place()
    return (d, lax.rem(c + dc, COLS), lax.rem(r + dr, ROWS))


def signal_entry(barrier):
    for dc, dr in OTHERS:
        pl.semaphore_signal(barrier, inc=1, device_id=peer(dc, dr), device_id_type=MESH)


def remote(ref, send, recv, to):
    return pltpu.make_async_remote_copy(
        src_ref=ref, dst_ref=ref, send_sem=send, recv_sem=recv, device_id=to, device_id_type=MESH)


def scalar_tile(s, w, r):
    rows = [jnp.sum(v, axis=0, keepdims=True) for v in (s, w, r)]
    return jnp.concatenate(rows + [jnp.zeros((1, LANES), F32)], axis=0)


def step_of(mat, buf, rel, clip):
    mt, nt = TOTALS[mat]
    tot = buf[0]
    for i in range(1, ROWS * COLS):
        tot = tot + buf[i]
    tot = jnp.sum(tot, axis=1, keepdims=True)
    s, w, r = tot[0:1, :], tot[1:2, :], tot[2:3, :]
    r_mean = r * (1.0 / (COLS * mt))
    u_rms = jnp.sqrt(s * (1.0 / (mt * nt)) * r_mean)
    w_rms = jnp.sqrt(w * (1.0 / (mt * nt)))
    step = rel * jnp.maximum(EPS_SCALE, w_rms)
    k = step * jnp.sqrt(r_mean) / jnp.maximum(1.0, u_rms / clip)
    return jnp.broadcast_to(k, (8, LANES))


def main_kernel(
    x_hbm, h_hbm, dg_hbm, du_hbm, do_hbm, wg_hbm, wu_hbm, wd_hbm,
    rg_hbm, cg_hbm, ru_hbm, cu_hbm, rd_hbm, cd_hbm, beta, rel, clip,
    gu, wu, wd, wg, rd_new, cd_new, rg_new, cg_new, ru_new, cu_new, kap, abc_u, bv_u,
    gd, gg, ring, xt, hs, ht, rowacc, abc_d, abc_g, cacc_d, cacc_g, cacc_u,
    bv_d, bv_g, rd, cd, rg, cg, ru, cu, rbuf_d, rbuf_g, rbuf_u, cbuf_d, cbuf_g, cbuf_u, sbuf, sacc, wacc,
    sem, r_send, r_recv, c_send, c_recv, s_send, s_recv,
):
    G, W = (gd, gg, gu), (wd, wg, wu)
    d_hbm, w_hbm = (do_hbm, dg_hbm, du_hbm), (wd_hbm, wg_hbm, wu_hbm)
    r_old, c_old = (rd, rg, ru), (cd, cg, cu)
    r_new, c_new = (rd_new, rg_new, ru_new), (cd_new, cg_new, cu_new)
    abc, cacc, bv = (abc_d, abc_g, abc_u), (cacc_d, cacc_g, cacc_u), (bv_d, bv_g, bv_u)
    rbuf, cbuf = (rbuf_d, rbuf_g, rbuf_u), (cbuf_d, cbuf_g, cbuf_u)
    _, me_c, me_r = place()

    def piece_copies(p):
        ks = slice(*PIECES[p])
        return (
            pltpu.make_async_copy(h_hbm.at[ks, :], hs.at[ks, :], sem.at[2 * p]),
            pltpu.make_async_copy(do_hbm.at[ks, :512], ring.at[0, ks, :512], sem.at[2 * p + 1]),
        )

    x_copy = pltpu.make_async_copy(x_hbm, ring.at[2, :, :512], sem.at[10])
    right_copy = pltpu.make_async_copy(do_hbm.at[:, 512:], ring.at[0, :, 512:], sem.at[11])

    places = (
        ring.at[1], hs.at[:, :1024], ring.at[2, :, :768],
        ring.at[0, :, :512], ring.at[1], ring.at[0, :, 512:1024], hs.at[:, :768],
    )

    def d_copy(j):
        mat, n0, n1 = BLOCKS[j]
        return pltpu.make_async_copy(d_hbm[mat].at[:, n0:n1], places[j], sem.at[(12, 13, 6, 7, 10, 8, 12)[j]])

    old_copies = [
        pltpu.make_async_copy(src, dst, sem.at[i])
        for i, (src, dst) in enumerate(zip((rd_hbm, cd_hbm, rg_hbm, cg_hbm, ru_hbm, cu_hbm), (rd, cd, rg, cg, ru, cu)))
    ]

    def w_copy(mat):
        return pltpu.make_async_copy(w_hbm[mat], W[mat], sem.at[(9, 11, 13)[mat]])

    late = slice(EARLY_COLS, SHAPES[UP][1] // LANES)
    COL_GROUPS = ((DOWN, slice(0, 8), 0), (GATE, slice(0, 22), 0), (UP, late, 0), (UP, slice(0, EARLY_COLS), 1))
    EARLY = 3

    def start_row(mat):
        row_copy(mat).start()

    def row_copy(mat):
        return remote(rbuf[mat].at[me_c], r_send.at[0], r_recv.at[mat], peer(1, 0))

    def start_cols(group):
        mat, part, send = COL_GROUPS[group]
        for d in (1, 2, 3):
            remote(cbuf[mat].at[me_r, part], c_send.at[send], c_recv.at[group], peer(0, d)).start()

    def all_cols(group):
        mat, part, send = COL_GROUPS[group]
        return remote(cbuf[mat].at[0:3, part], c_send.at[send], c_recv.at[group], peer(0, 1))

    def start_tiles(mat):
        me = me_c * ROWS + me_r
        for dc, dr in OTHERS:
            remote(sbuf.at[mat, me], s_send.at[0], s_recv.at[mat], peer(dc, dr)).start()

    def all_tiles(mat):
        return remote(sbuf.at[mat, 0:7], s_send.at[0], s_recv.at[mat], peer(0, 1))

    def start(copies):
        for c in copies:
            c.start()

    def wait(copies):
        for c in copies:
            c.wait()

    def stats_units(mat, n0, n1):
        units = []
        for r in range(0, SHAPES[mat][0], CHUNK):
            def unit(r=r):
                part = None
                for t in range(n0 // LANES, n1 // LANES):
                    g = G[mat][r:r + CHUNK, t * LANES:(t + 1) * LANES]
                    q = g * g
                    part = q if part is None else part + q
                    col = fold(q)
                    cols = pl.ds(t * LANES, LANES)
                    cacc[mat][:, cols] = col if r == 0 else cacc[mat][:, cols] + col
                rows = pl.ds(r, CHUNK)
                rowacc[rows, :] = part if n0 == 0 else rowacc[rows, :] + part
            units.append(unit)
        return units

    def row_units(mat):
        units = []
        for i in range(SHAPES[mat][0] // LANES):
            def rows(i=i):
                block = rowacc[i * LANES:(i + 1) * LANES, :].T
                rbuf[mat][me_c, i:i + 1, :] = jnp.sum(block, axis=0, keepdims=True)
            units.append(rows)
        return units

    def col_units(mat, t0, t1):
        units = []
        for t in range(t0, t1):
            def cols(t=t):
                cbuf[mat][me_r, t:t + 1, :] = jnp.sum(
                    cacc[mat][:, t * LANES:(t + 1) * LANES], axis=0, keepdims=True)
            units.append(cols)
        return units

    def sums_units(mat):
        return row_units(mat) + col_units(mat, 0, SHAPES[mat][1] // LANES)

    def w2_units(mat):
        units = []
        m, n = SHAPES[mat]
        for i in range(m // CHUNK):
            def unit(i=i):
                acc = None
                for t in range(n // LANES):
                    w = W[mat][i * CHUNK:(i + 1) * CHUNK, t * LANES:(t + 1) * LANES]
                    f = fold(w * w)
                    acc = f if acc is None else acc + f
                wacc[mat, i] = acc
            units.append(unit)
        return units

    def factor_units(mat):
        m, n = SHAPES[mat]
        mt, nt = TOTALS[mat]

        def new():
            b2 = beta[0]
            rows = rbuf[mat][0] + rbuf[mat][1]
            cols = (cbuf[mat][0] + cbuf[mat][1]) + (cbuf[mat][2] + cbuf[mat][3])
            rn = b2 * r_old[mat][...] + (1.0 - b2) * (rows * (1.0 / nt) + EPS_SQ)
            cn = b2 * c_old[mat][...] + (1.0 - b2) * (cols * (1.0 / mt) + EPS_SQ)
            r_new[mat][...] = rn
            c_new[mat][...] = cn
            bv[mat][...] = lax.rsqrt(cn)

        units = [new]
        for i in range(m // LANES):
            def unit(i=i):
                a = lax.rsqrt(r_new[mat][i:i + 1, :])
                abc[mat][i * LANES:(i + 1) * LANES, :] = jnp.broadcast_to(a, (LANES, LANES)).T
            units.append(unit)
        return units

    def scale_units(mat):
        units = []
        m, n = SHAPES[mat]
        for i in range(m // CHUNK):
            def unit(i=i):
                acc = None
                rows = slice(i * CHUNK, (i + 1) * CHUNK)
                for t in range(n // LANES):
                    h = G[mat][rows, t * LANES:(t + 1) * LANES] * bv[mat][t:t + 1, :]
                    acc = h * h if acc is None else acc + h * h
                a = abc[mat][rows, :]
                sacc[mat, i] = fold(acc * (a * a))
            units.append(unit)
        return units

    def update_units(mat):
        def step():
            kap[mat] = step_of(mat, sbuf.at[mat], rel[0], clip[0])

        units = [step]
        m, n = SHAPES[mat]
        for r in range(0, m, CHUNK):
            def unit(r=r):
                ka = abc[mat][r:r + CHUNK, :] * kap[mat, 0:1, :]
                for t in range(n // LANES):
                    cols = slice(t * LANES, (t + 1) * LANES)
                    W[mat][r:r + CHUNK, cols] = (
                        W[mat][r:r + CHUNK, cols] - G[mat][r:r + CHUNK, cols] * ka * bv[mat][t:t + 1, :])
            units.append(unit)
        return units

    def tile_unit(mat):
        def unit():
            _, c, r = place()
            chunks = SHAPES[mat][0] // CHUNK
            sbuf[mat, c * ROWS + r] = scalar_tile(
                jnp.sum(sacc[mat, :chunks], axis=0), jnp.sum(wacc[mat, :chunks], axis=0), r_new[mat][...])
        return [unit]

    def h_units(p):
        k0, k1 = PIECES[p]
        units = []
        for k in range(k0, k1, 256):
            for i in range(0, SHAPES[DOWN][0], LANES):
                def unit(k=k, i=i):
                    ht[i:i + LANES, k:k + 256] = hs[k:k + 256, i:i + LANES].T
                units.append(unit)
        return units

    def x_units():
        units = []
        for k in range(0, K, 256):
            for i in range(0, 512, LANES):
                def unit(k=k, i=i):
                    xt[i:i + LANES, k:k + 256] = ring[2, k:k + 256, i:i + LANES].T
                units.append(unit)
        return units

    def down_dots(p):
        ks = slice(*PIECES[p])
        out = []
        for r in range(0, 1408, 352):
            def dot(r=r):
                rs = slice(r, r + 352)
                part = jnp.dot(ht[rs, ks], ring[0, ks, :512], preferred_element_type=F32)
                gd[rs, :512] = part if p == 0 else gd[rs, :512] + part
            out.append(dot)
        return out

    def right_dots():
        out = []
        for r in range(0, 1408, 352):
            def dot(r=r):
                rs = slice(r, r + 352)
                gd[rs, 512:] = jnp.dot(ht[rs, :], ring[0, :, 512:], preferred_element_type=F32)
            out.append(dot)
        return out

    def dots_of(j):
        mat, n0, n1 = BLOCKS[j]
        out = []

        def dot(r0, r1, c0, c1):
            def run():
                G[mat][r0:r1, n0 + c0:n0 + c1] = jnp.dot(
                    xt[r0:r1, :], places[j][:, c0:c1], preferred_element_type=F32)
            return run

        w = n1 - n0
        for c in range(0, w, 512):
            if c + 512 <= w:
                out.append(dot(0, 512, c, c + 512))
            else:
                out += [dot(0, 256, c, w), dot(256, 512, c, w)]
        return out

    def run(units):
        for unit in units:
            unit()

    for p in (0, 1, 2):
        start(piece_copies(p))
    barrier = pltpu.get_barrier_semaphore()
    signal_entry(barrier)
    wait(piece_copies(0))
    start(piece_copies(3))
    start(piece_copies(4))
    right_copy.start()
    x_copy.start()
    run(h_units(0))
    for p in range(4):
        wait(piece_copies(p + 1))
        if p == 1:
            d_copy(0).start()
        interleave(down_dots(p), h_units(p + 1))
    d_copy(1).start()
    interleave(down_dots(4), [])
    start(old_copies)
    right_copy.wait()
    x_copy.wait()
    interleave(right_dots(), x_units() + stats_units(DOWN, 0, 512))
    d_copy(2).start()
    d_copy(3).start()
    d_copy(5).start()
    w_copy(DOWN).start()

    d_copy(0).wait()
    wait(old_copies)
    interleave(dots_of(0), stats_units(DOWN, 512, 1024) + sums_units(DOWN))
    pl.semaphore_wait(barrier, len(OTHERS))
    start_row(DOWN)
    start_cols(DOWN)
    d_copy(4).start()
    w_copy(GATE).start()

    d_copy(1).wait()
    d_copy(2).wait()
    interleave(dots_of(1), stats_units(GATE, 0, 1024))
    interleave(dots_of(2), stats_units(GATE, 1024, 2048))
    d_copy(6).start()
    w_copy(UP).start()

    d_copy(3).wait()
    interleave(dots_of(3), stats_units(GATE, 2048, 2816) + sums_units(GATE))
    row_copy(DOWN).wait_send()
    all_cols(DOWN).wait_send()
    start_row(GATE)
    start_cols(GATE)

    d_copy(4).wait()
    d_copy(5).wait()
    row_copy(DOWN).wait_recv()
    all_cols(DOWN).wait_recv()
    interleave(dots_of(4) + dots_of(5), stats_units(UP, 0, 512) + factor_units(DOWN) + scale_units(DOWN))

    d_copy(6).wait()
    interleave(dots_of(6), stats_units(UP, 512, 1536) + stats_units(UP, 1536, 2048) + col_units(UP, 0, EARLY_COLS))
    start_cols(EARLY)

    run(stats_units(UP, 2048, 2816) + row_units(UP) + col_units(UP, EARLY_COLS, 22))
    row_copy(GATE).wait_send()
    all_cols(GATE).wait_send()
    start_row(UP)
    start_cols(UP)
    w_copy(DOWN).wait()
    w_copy(GATE).wait()
    w_copy(UP).wait()
    run(w2_units(DOWN) + tile_unit(DOWN))
    start_tiles(DOWN)
    row_copy(GATE).wait_recv()
    all_cols(GATE).wait_recv()
    run(factor_units(GATE) + scale_units(GATE) + w2_units(GATE) + tile_unit(GATE))
    all_tiles(DOWN).wait_send()
    start_tiles(GATE)
    run(w2_units(UP))
    all_cols(EARLY).wait_recv()
    row_copy(UP).wait_recv()
    all_cols(UP).wait_recv()
    run(factor_units(UP) + scale_units(UP) + tile_unit(UP))
    all_tiles(GATE).wait_send()
    start_tiles(UP)
    all_tiles(DOWN).wait_recv()
    run(update_units(DOWN))
    all_tiles(GATE).wait_recv()
    run(update_units(GATE))
    row_copy(UP).wait_send()
    all_cols(UP).wait_send()
    all_cols(EARLY).wait_send()
    all_tiles(UP).wait_send()
    all_tiles(UP).wait_recv()
    kap[UP] = step_of(UP, sbuf.at[UP], rel[0], clip[0])


def update_kernel(
    gu, wu, wd, wg, rd, cd, rg, cg, ru, cu, kap, abc, bv,
    wu_o, wd_o, wg_o, rd_o, cd_o, rg_o, cg_o, ru_o, cu_o, stage, sem,
):
    srcs = (wd, wg, rd, cd, rg, cg, ru, cu)
    dsts = (wd_o, wg_o, rd_o, cd_o, rg_o, cg_o, ru_o, cu_o)
    copies = [pltpu.make_async_copy(src, dst, sem) for src, dst in zip(srcs, dsts)]
    for c in copies:
        c.start()
    m, n = SHAPES[UP]
    k = kap[UP, 0:1, :]
    for r in range(0, m, CHUNK):
        ka = abc[r:r + CHUNK, :] * k
        for t in range(n // LANES):
            cols = slice(t * LANES, (t + 1) * LANES)
            stage[r:r + CHUNK, cols] = wu[r:r + CHUNK, cols] - gu[r:r + CHUNK, cols] * ka * bv[t:t + 1, :]
        copies.append(pltpu.make_async_copy(stage.at[r:r + CHUNK, :], wu_o.at[r:r + CHUNK, :], sem))
        copies[-1].start()
    for copy in copies:
        copy.wait()


VMEM_LIMIT = 41 * 1024 * 1024


def local_program(x_in, h_act, d_gate, d_up, d_out, w_gate, w_up, w_down, r_gate, c_gate, r_up, c_up, r_down, c_down, beta_two, rel_step, clip_thr):
    any_spec = pl.BlockSpec(memory_space=pl.ANY)
    vmem_spec = pl.BlockSpec(memory_space=pltpu.VMEM)
    smem_spec = pl.BlockSpec(memory_space=pltpu.SMEM)

    def stat_shape(v):
        return (v // LANES, LANES)

    stats = [v.reshape(stat_shape(v.shape[0])) for v in (r_gate, c_gate, r_up, c_up, r_down, c_down)]
    beta, rel, clip = [v.reshape(1) for v in (beta_two, rel_step, clip_thr)]
    rows = [stat_shape(m) for m, n in SHAPES]
    cols = [stat_shape(n) for m, n in SHAPES]
    dma = pltpu.SemaphoreType.DMA

    stat_pairs = [s for pair in zip(rows, cols) for s in pair]
    outs = pl.pallas_call(
        main_kernel,
        out_shape=[pltpu.VMEM(SHAPES[UP], F32)] * 2 + [pltpu.VMEM(s, F32) for s in SHAPES[:2]]
        + [pltpu.VMEM(s, F32) for s in stat_pairs]
        + [pltpu.VMEM((3, 8, LANES), F32), pltpu.VMEM((512, LANES), F32), pltpu.VMEM(cols[UP], F32)],
        in_specs=[any_spec] * 14 + [smem_spec] * 3,
        out_specs=[vmem_spec] * 13,
        scratch_shapes=[
            pltpu.VMEM(SHAPES[DOWN], F32),
            pltpu.VMEM(SHAPES[GATE], F32),
            pltpu.VMEM((3, K, 1024), BF16),
            pltpu.VMEM((512, K), BF16),
            pltpu.VMEM((K, 1408), BF16),
            pltpu.VMEM((1408, K), BF16),
            pltpu.VMEM((1408, LANES), F32),
            pltpu.VMEM((1408, LANES), F32),
            pltpu.VMEM((512, LANES), F32),
        ]
        + [pltpu.VMEM((8, n), F32) for m, n in SHAPES]
        + [pltpu.VMEM(s, F32) for s in cols[:2]]
        + [pltpu.VMEM(s, F32) for s in stat_pairs]
        + [pltpu.VMEM((COLS, *s), F32) for s in rows]
        + [pltpu.VMEM((ROWS, *s), F32) for s in cols]
        + [
            pltpu.VMEM((3, ROWS * COLS, 4, LANES), F32),
            pltpu.VMEM((3, 22, 8, LANES), F32),
            pltpu.VMEM((3, 22, 8, LANES), F32),
            dma((14,)), dma((1,)), dma((3,)), dma((2,)), dma((4,)), dma((1,)), dma((3,)),
        ],
        compiler_params=pltpu.CompilerParams(
            collective_id=0, has_side_effects=True, vmem_limit_bytes=VMEM_LIMIT),
        name="main",
    )(
        *[pltpu.with_memory_space_constraint(v, pltpu.HBM)
          for v in (x_in, h_act, d_gate, d_up, d_out, w_gate, w_up, w_down, *stats)],
        beta, rel, clip)
    held = [pltpu.with_memory_space_constraint(v, pltpu.VMEM) for v in outs]
    res = pl.pallas_call(
        update_kernel,
        out_shape=[jax.ShapeDtypeStruct(s, F32) for s in (SHAPES[UP], *SHAPES[:2], *stat_pairs)],
        in_specs=[vmem_spec] * 13,
        out_specs=[any_spec] * 9,
        scratch_shapes=[pltpu.VMEM(SHAPES[UP], F32), dma],
        compiler_params=pltpu.CompilerParams(vmem_limit_bytes=VMEM_LIMIT),
        name="update",
    )(*held)
    up, down, gate, rd_n, cd_n, rg_n, cg_n, ru_n, cu_n = res
    flat = [v.reshape(-1) for v in (rg_n, cg_n, ru_n, cu_n, rd_n, cd_n)]
    return (gate, up, down, *flat)


def solution(mesh):
    act_spec = P(None, "row")
    cot_spec = P(None, "col")
    w_spec = P("row", "col")
    r_spec = P("row")
    c_spec = P("col")
    s_spec = P()
    return jax.shard_map(local_program, mesh=mesh, in_specs=(act_spec, act_spec, cot_spec, cot_spec, cot_spec, w_spec, w_spec, w_spec, r_spec, c_spec, r_spec, c_spec, r_spec, c_spec, s_spec, s_spec, s_spec), out_specs=(w_spec, w_spec, w_spec, r_spec, c_spec, r_spec, c_spec, r_spec, c_spec), check_vma=False)
```

```python
import jax
import jax.numpy as jnp
from jax import lax
from jax.experimental import pallas as pl
from jax.experimental.pallas import tpu as pltpu
from jax.sharding import PartitionSpec as P

EPS_SQ = 1e-30
EPS_SCALE = 1e-3
LANES = 128
K = 2048
ROWS, COLS = 4, 2
F32 = jnp.float32
BF16 = jnp.bfloat16
MESH = pl.DeviceIdType.MESH

DOWN, GATE, UP = 0, 1, 2
SHAPES = ((1408, 1024), (512, 2816), (512, 2816))
TOTALS = tuple((m * ROWS, n * COLS) for m, n in SHAPES)
PIECES = ((0, 256), (256, 512), (512, 1024), (1024, 1536), (1536, 2048))
GATE_BLOCKS = ((0, 1024), (1024, 2048), (2048, 2816))
UP_BLOCKS = ((0, 512), (512, 1536), (1536, 2048), (2048, 2816))
BLOCKS = tuple((GATE, *b) for b in GATE_BLOCKS) + tuple((UP, *b) for b in UP_BLOCKS)
EARLY_COLS = 16
CHUNK = 64
OTHERS = [(dc, dr) for dc in range(COLS) for dr in range(ROWS) if (dc, dr) != (0, 0)]


def interleave(dots, units):
    done = 0
    for i, dot in enumerate(dots):
        upto = len(units) * (i + 1) // len(dots)
        for unit in units[done:upto]:
            unit()
        done = upto
        dot()


def fold(x):
    return jnp.sum(x.reshape(x.shape[0] // 8, 8, x.shape[1]), axis=0)


def place():
    return lax.axis_index("data"), lax.axis_index("col"), lax.axis_index("row")


def peer(dc, dr):
    d, c, r = place()
    return (d, lax.rem(c + dc, COLS), lax.rem(r + dr, ROWS))


def signal_entry(barrier):
    for dc, dr in OTHERS:
        pl.semaphore_signal(barrier, inc=1, device_id=peer(dc, dr), device_id_type=MESH)


def remote(ref, send, recv, to):
    return pltpu.make_async_remote_copy(
        src_ref=ref, dst_ref=ref, send_sem=send, recv_sem=recv, device_id=to, device_id_type=MESH)


def scalar_tile(s, w, r):
    rows = [jnp.sum(v, axis=0, keepdims=True) for v in (s, w, r)]
    return jnp.concatenate(rows + [jnp.zeros((1, LANES), F32)], axis=0)


def step_of(mat, buf, rel, clip):
    mt, nt = TOTALS[mat]
    tot = buf[0]
    for i in range(1, ROWS * COLS):
        tot = tot + buf[i]
    tot = jnp.sum(tot, axis=1, keepdims=True)
    s, w, r = tot[0:1, :], tot[1:2, :], tot[2:3, :]
    r_mean = r * (1.0 / (COLS * mt))
    u_rms = jnp.sqrt(s * (1.0 / (mt * nt)) * r_mean)
    w_rms = jnp.sqrt(w * (1.0 / (mt * nt)))
    step = rel * jnp.maximum(EPS_SCALE, w_rms)
    k = step * jnp.sqrt(r_mean) / jnp.maximum(1.0, u_rms / clip)
    return jnp.broadcast_to(k, (8, LANES))


def main_kernel(
    x_hbm, h_hbm, dg_hbm, du_hbm, do_hbm, wg_hbm, wu_hbm, wd_hbm,
    rg_hbm, cg_hbm, ru_hbm, cu_hbm, rd_hbm, cd_hbm, beta, rel, clip,
    gu, wu, wd, wg, rd_new, cd_new, rg_new, cg_new, ru_new, cu_new, kap, abc_u, bv_u,
    gd, gg, ring, xt, hs, ht, rowacc, abc_d, abc_g, cacc_d, cacc_g, cacc_u,
    bv_d, bv_g, rd, cd, rg, cg, ru, cu, rbuf_d, rbuf_g, rbuf_u, cbuf_d, cbuf_g, cbuf_u, sbuf, sacc, wacc,
    sem, r_send, r_recv, c_send, c_recv, s_send, s_recv,
):
    G, W = (gd, gg, gu), (wd, wg, wu)
    d_hbm, w_hbm = (do_hbm, dg_hbm, du_hbm), (wd_hbm, wg_hbm, wu_hbm)
    r_old, c_old = (rd, rg, ru), (cd, cg, cu)
    r_new, c_new = (rd_new, rg_new, ru_new), (cd_new, cg_new, cu_new)
    abc, cacc, bv = (abc_d, abc_g, abc_u), (cacc_d, cacc_g, cacc_u), (bv_d, bv_g, bv_u)
    rbuf, cbuf = (rbuf_d, rbuf_g, rbuf_u), (cbuf_d, cbuf_g, cbuf_u)
    _, me_c, me_r = place()

    def piece_copies(p):
        ks = slice(*PIECES[p])
        return (
            pltpu.make_async_copy(h_hbm.at[ks, :], hs.at[ks, :], sem.at[2 * p]),
            pltpu.make_async_copy(do_hbm.at[ks, :512], ring.at[0, ks, :512], sem.at[2 * p + 1]),
        )

    x_copy = pltpu.make_async_copy(x_hbm, ring.at[2, :, :512], sem.at[10])
    right_copy = pltpu.make_async_copy(do_hbm.at[:, 512:], ring.at[0, :, 512:], sem.at[11])

    places = (
        ring.at[1], hs.at[:, :1024], ring.at[2, :, :768],
        ring.at[0, :, :512], ring.at[1], ring.at[0, :, 512:1024], hs.at[:, :768],
    )

    def d_copy(j):
        mat, n0, n1 = BLOCKS[j]
        return pltpu.make_async_copy(d_hbm[mat].at[:, n0:n1], places[j], sem.at[(12, 13, 6, 7, 10, 8, 12)[j]])

    old_copies = [
        pltpu.make_async_copy(src, dst, sem.at[i])
        for i, (src, dst) in enumerate(zip((rd_hbm, cd_hbm, rg_hbm, cg_hbm, ru_hbm, cu_hbm), (rd, cd, rg, cg, ru, cu)))
    ]

    def w_copy(mat):
        return pltpu.make_async_copy(w_hbm[mat], W[mat], sem.at[(9, 11, 13)[mat]])

    late = slice(EARLY_COLS, SHAPES[UP][1] // LANES)
    COL_GROUPS = ((DOWN, slice(0, 8), 0), (GATE, slice(0, 22), 0), (UP, late, 0), (UP, slice(0, EARLY_COLS), 1))
    EARLY = 3

    def start_row(mat):
        row_copy(mat).start()

    def row_copy(mat):
        return remote(rbuf[mat].at[me_c], r_send.at[0], r_recv.at[mat], peer(1, 0))

    def start_cols(group):
        mat, part, send = COL_GROUPS[group]
        for d in (1, 2, 3):
            remote(cbuf[mat].at[me_r, part], c_send.at[send], c_recv.at[group], peer(0, d)).start()

    def all_cols(group):
        mat, part, send = COL_GROUPS[group]
        return remote(cbuf[mat].at[0:3, part], c_send.at[send], c_recv.at[group], peer(0, 1))

    def start_tiles(mat):
        me = me_c * ROWS + me_r
        for dc, dr in OTHERS:
            remote(sbuf.at[mat, me], s_send.at[0], s_recv.at[mat], peer(dc, dr)).start()

    def all_tiles(mat):
        return remote(sbuf.at[mat, 0:7], s_send.at[0], s_recv.at[mat], peer(0, 1))

    def start(copies):
        for c in copies:
            c.start()

    def wait(copies):
        for c in copies:
            c.wait()

    def stats_units(mat, n0, n1):
        units = []
        for r in range(0, SHAPES[mat][0], CHUNK):
            def unit(r=r):
                part = None
                for t in range(n0 // LANES, n1 // LANES):
                    g = G[mat][r:r + CHUNK, t * LANES:(t + 1) * LANES]
                    q = g * g
                    part = q if part is None else part + q
                    col = fold(q)
                    cols = pl.ds(t * LANES, LANES)
                    cacc[mat][:, cols] = col if r == 0 else cacc[mat][:, cols] + col
                rows = pl.ds(r, CHUNK)
                rowacc[rows, :] = part if n0 == 0 else rowacc[rows, :] + part
            units.append(unit)
        return units

    def row_units(mat):
        units = []
        for i in range(SHAPES[mat][0] // LANES):
            def rows(i=i):
                block = rowacc[i * LANES:(i + 1) * LANES, :].T
                rbuf[mat][me_c, i:i + 1, :] = jnp.sum(block, axis=0, keepdims=True)
            units.append(rows)
        return units

    def col_units(mat, t0, t1):
        units = []
        for t in range(t0, t1):
            def cols(t=t):
                cbuf[mat][me_r, t:t + 1, :] = jnp.sum(
                    cacc[mat][:, t * LANES:(t + 1) * LANES], axis=0, keepdims=True)
            units.append(cols)
        return units

    def sums_units(mat):
        return row_units(mat) + col_units(mat, 0, SHAPES[mat][1] // LANES)

    def w2_units(mat):
        units = []
        m, n = SHAPES[mat]
        for i in range(m // CHUNK):
            def unit(i=i):
                acc = None
                for t in range(n // LANES):
                    w = W[mat][i * CHUNK:(i + 1) * CHUNK, t * LANES:(t + 1) * LANES]
                    f = fold(w * w)
                    acc = f if acc is None else acc + f
                wacc[mat, i] = acc
            units.append(unit)
        return units

    def factor_units(mat):
        m, n = SHAPES[mat]
        mt, nt = TOTALS[mat]

        def new():
            b2 = beta[0]
            rows = rbuf[mat][0] + rbuf[mat][1]
            cols = (cbuf[mat][0] + cbuf[mat][1]) + (cbuf[mat][2] + cbuf[mat][3])
            rn = b2 * r_old[mat][...] + (1.0 - b2) * (rows * (1.0 / nt) + EPS_SQ)
            cn = b2 * c_old[mat][...] + (1.0 - b2) * (cols * (1.0 / mt) + EPS_SQ)
            r_new[mat][...] = rn
            c_new[mat][...] = cn
            bv[mat][...] = lax.rsqrt(cn)

        units = [new]
        for i in range(m // LANES):
            def unit(i=i):
                a = lax.rsqrt(r_new[mat][i:i + 1, :])
                abc[mat][i * LANES:(i + 1) * LANES, :] = jnp.broadcast_to(a, (LANES, LANES)).T
            units.append(unit)
        return units

    def scale_units(mat):
        units = []
        m, n = SHAPES[mat]
        for i in range(m // CHUNK):
            def unit(i=i):
                acc = None
                rows = slice(i * CHUNK, (i + 1) * CHUNK)
                for t in range(n // LANES):
                    h = G[mat][rows, t * LANES:(t + 1) * LANES] * bv[mat][t:t + 1, :]
                    acc = h * h if acc is None else acc + h * h
                a = abc[mat][rows, :]
                sacc[mat, i] = fold(acc * (a * a))
            units.append(unit)
        return units

    def update_units(mat):
        def step():
            kap[mat] = step_of(mat, sbuf.at[mat], rel[0], clip[0])

        units = [step]
        m, n = SHAPES[mat]
        for r in range(0, m, CHUNK):
            def unit(r=r):
                ka = abc[mat][r:r + CHUNK, :] * kap[mat, 0:1, :]
                for t in range(n // LANES):
                    cols = slice(t * LANES, (t + 1) * LANES)
                    W[mat][r:r + CHUNK, cols] = (
                        W[mat][r:r + CHUNK, cols] - G[mat][r:r + CHUNK, cols] * ka * bv[mat][t:t + 1, :])
            units.append(unit)
        return units

    def tile_unit(mat):
        def unit():
            _, c, r = place()
            chunks = SHAPES[mat][0] // CHUNK
            sbuf[mat, c * ROWS + r] = scalar_tile(
                jnp.sum(sacc[mat, :chunks], axis=0), jnp.sum(wacc[mat, :chunks], axis=0), r_new[mat][...])
        return [unit]

    def h_units(p):
        k0, k1 = PIECES[p]
        units = []
        for k in range(k0, k1, 256):
            for i in range(0, SHAPES[DOWN][0], LANES):
                def unit(k=k, i=i):
                    ht[i:i + LANES, k:k + 256] = hs[k:k + 256, i:i + LANES].T
                units.append(unit)
        return units

    def x_units():
        units = []
        for k in range(0, K, 256):
            for i in range(0, 512, LANES):
                def unit(k=k, i=i):
                    xt[i:i + LANES, k:k + 256] = ring[2, k:k + 256, i:i + LANES].T
                units.append(unit)
        return units

    def down_dots(p):
        ks = slice(*PIECES[p])
        out = []
        for r in range(0, 1408, 352):
            def dot(r=r):
                rs = slice(r, r + 352)
                part = jnp.dot(ht[rs, ks], ring[0, ks, :512], preferred_element_type=F32)
                gd[rs, :512] = part if p == 0 else gd[rs, :512] + part
            out.append(dot)
        return out

    def right_dots():
        out = []
        for r in range(0, 1408, 352):
            def dot(r=r):
                rs = slice(r, r + 352)
                gd[rs, 512:] = jnp.dot(ht[rs, :], ring[0, :, 512:], preferred_element_type=F32)
            out.append(dot)
        return out

    def dots_of(j):
        mat, n0, n1 = BLOCKS[j]
        out = []

        def dot(r0, r1, c0, c1):
            def run():
                G[mat][r0:r1, n0 + c0:n0 + c1] = jnp.dot(
                    xt[r0:r1, :], places[j][:, c0:c1], preferred_element_type=F32)
            return run

        w = n1 - n0
        for c in range(0, w, 512):
            if c + 512 <= w:
                out.append(dot(0, 512, c, c + 512))
            else:
                out += [dot(0, 256, c, w), dot(256, 512, c, w)]
        return out

    def run(units):
        for unit in units:
            unit()

    for p in (0, 1, 2):
        start(piece_copies(p))
    barrier = pltpu.get_barrier_semaphore()
    signal_entry(barrier)
    wait(piece_copies(0))
    start(piece_copies(3))
    start(piece_copies(4))
    right_copy.start()
    x_copy.start()
    run(h_units(0))
    for p in range(4):
        wait(piece_copies(p + 1))
        if p == 1:
            d_copy(0).start()
        interleave(down_dots(p), h_units(p + 1))
    d_copy(1).start()
    interleave(down_dots(4), [])
    start(old_copies)
    right_copy.wait()
    x_copy.wait()
    interleave(right_dots(), x_units() + stats_units(DOWN, 0, 512))
    d_copy(2).start()
    d_copy(3).start()
    d_copy(5).start()
    w_copy(DOWN).start()

    d_copy(0).wait()
    wait(old_copies)
    interleave(dots_of(0), stats_units(DOWN, 512, 1024) + sums_units(DOWN))
    pl.semaphore_wait(barrier, len(OTHERS))
    start_row(DOWN)
    start_cols(DOWN)
    d_copy(4).start()
    w_copy(GATE).start()

    d_copy(1).wait()
    d_copy(2).wait()
    interleave(dots_of(1), stats_units(GATE, 0, 1024))
    interleave(dots_of(2), stats_units(GATE, 1024, 2048))
    d_copy(6).start()
    w_copy(UP).start()

    d_copy(3).wait()
    w_copy(DOWN).wait()
    interleave(dots_of(3), stats_units(GATE, 2048, 2816) + sums_units(GATE) + w2_units(DOWN)[:11])
    row_copy(DOWN).wait_send()
    all_cols(DOWN).wait_send()
    start_row(GATE)
    start_cols(GATE)

    d_copy(4).wait()
    d_copy(5).wait()
    row_copy(DOWN).wait_recv()
    all_cols(DOWN).wait_recv()
    interleave(dots_of(4) + dots_of(5), stats_units(UP, 0, 512) + factor_units(DOWN) + scale_units(DOWN) + w2_units(DOWN)[11:])

    d_copy(6).wait()
    interleave(
        dots_of(6),
        tile_unit(DOWN) + stats_units(UP, 512, 1536) + stats_units(UP, 1536, 2048) + col_units(UP, 0, EARLY_COLS))
    start_cols(EARLY)
    start_tiles(DOWN)

    run(stats_units(UP, 2048, 2816) + row_units(UP) + col_units(UP, EARLY_COLS, 22))
    row_copy(GATE).wait_send()
    all_cols(GATE).wait_send()
    start_row(UP)
    start_cols(UP)
    w_copy(GATE).wait()
    w_copy(UP).wait()
    row_copy(GATE).wait_recv()
    all_cols(GATE).wait_recv()
    run(factor_units(GATE) + scale_units(GATE) + w2_units(GATE) + tile_unit(GATE))
    all_tiles(DOWN).wait_send()
    start_tiles(GATE)
    run(w2_units(UP))
    all_cols(EARLY).wait_recv()
    row_copy(UP).wait_recv()
    all_cols(UP).wait_recv()
    run(factor_units(UP) + scale_units(UP) + tile_unit(UP))
    all_tiles(GATE).wait_send()
    start_tiles(UP)
    all_tiles(DOWN).wait_recv()
    run(update_units(DOWN))
    all_tiles(GATE).wait_recv()
    run(update_units(GATE))
    row_copy(UP).wait_send()
    all_cols(UP).wait_send()
    all_cols(EARLY).wait_send()
    all_tiles(UP).wait_send()
    all_tiles(UP).wait_recv()
    kap[UP] = step_of(UP, sbuf.at[UP], rel[0], clip[0])


def update_kernel(
    gu, wu, wd, wg, rd, cd, rg, cg, ru, cu, kap, abc, bv,
    wu_o, wd_o, wg_o, rd_o, cd_o, rg_o, cg_o, ru_o, cu_o, stage, sem,
):
    srcs = (wd, wg, rd, cd, rg, cg, ru, cu)
    dsts = (wd_o, wg_o, rd_o, cd_o, rg_o, cg_o, ru_o, cu_o)
    copies = [pltpu.make_async_copy(src, dst, sem) for src, dst in zip(srcs, dsts)]
    for c in copies:
        c.start()
    m, n = SHAPES[UP]
    k = kap[UP, 0:1, :]
    for r in range(0, m, CHUNK):
        ka = abc[r:r + CHUNK, :] * k
        for t in range(n // LANES):
            cols = slice(t * LANES, (t + 1) * LANES)
            stage[r:r + CHUNK, cols] = wu[r:r + CHUNK, cols] - gu[r:r + CHUNK, cols] * ka * bv[t:t + 1, :]
        copies.append(pltpu.make_async_copy(stage.at[r:r + CHUNK, :], wu_o.at[r:r + CHUNK, :], sem))
        copies[-1].start()
    for copy in copies:
        copy.wait()


VMEM_LIMIT = 41 * 1024 * 1024


def local_program(x_in, h_act, d_gate, d_up, d_out, w_gate, w_up, w_down, r_gate, c_gate, r_up, c_up, r_down, c_down, beta_two, rel_step, clip_thr):
    any_spec = pl.BlockSpec(memory_space=pl.ANY)
    vmem_spec = pl.BlockSpec(memory_space=pltpu.VMEM)
    smem_spec = pl.BlockSpec(memory_space=pltpu.SMEM)

    def stat_shape(v):
        return (v // LANES, LANES)

    stats = [v.reshape(stat_shape(v.shape[0])) for v in (r_gate, c_gate, r_up, c_up, r_down, c_down)]
    beta, rel, clip = [v.reshape(1) for v in (beta_two, rel_step, clip_thr)]
    rows = [stat_shape(m) for m, n in SHAPES]
    cols = [stat_shape(n) for m, n in SHAPES]
    dma = pltpu.SemaphoreType.DMA

    stat_pairs = [s for pair in zip(rows, cols) for s in pair]
    outs = pl.pallas_call(
        main_kernel,
        out_shape=[pltpu.VMEM(SHAPES[UP], F32)] * 2 + [pltpu.VMEM(s, F32) for s in SHAPES[:2]]
        + [pltpu.VMEM(s, F32) for s in stat_pairs]
        + [pltpu.VMEM((3, 8, LANES), F32), pltpu.VMEM((512, LANES), F32), pltpu.VMEM(cols[UP], F32)],
        in_specs=[any_spec] * 14 + [smem_spec] * 3,
        out_specs=[vmem_spec] * 13,
        scratch_shapes=[
            pltpu.VMEM(SHAPES[DOWN], F32),
            pltpu.VMEM(SHAPES[GATE], F32),
            pltpu.VMEM((3, K, 1024), BF16),
            pltpu.VMEM((512, K), BF16),
            pltpu.VMEM((K, 1408), BF16),
            pltpu.VMEM((1408, K), BF16),
            pltpu.VMEM((1408, LANES), F32),
            pltpu.VMEM((1408, LANES), F32),
            pltpu.VMEM((512, LANES), F32),
        ]
        + [pltpu.VMEM((8, n), F32) for m, n in SHAPES]
        + [pltpu.VMEM(s, F32) for s in cols[:2]]
        + [pltpu.VMEM(s, F32) for s in stat_pairs]
        + [pltpu.VMEM((COLS, *s), F32) for s in rows]
        + [pltpu.VMEM((ROWS, *s), F32) for s in cols]
        + [
            pltpu.VMEM((3, ROWS * COLS, 4, LANES), F32),
            pltpu.VMEM((3, 22, 8, LANES), F32),
            pltpu.VMEM((3, 22, 8, LANES), F32),
            dma((14,)), dma((1,)), dma((3,)), dma((2,)), dma((4,)), dma((1,)), dma((3,)),
        ],
        compiler_params=pltpu.CompilerParams(
            collective_id=0, has_side_effects=True, vmem_limit_bytes=VMEM_LIMIT),
        name="main",
    )(
        *[pltpu.with_memory_space_constraint(v, pltpu.HBM)
          for v in (x_in, h_act, d_gate, d_up, d_out, w_gate, w_up, w_down, *stats)],
        beta, rel, clip)
    held = [pltpu.with_memory_space_constraint(v, pltpu.VMEM) for v in outs]
    res = pl.pallas_call(
        update_kernel,
        out_shape=[jax.ShapeDtypeStruct(s, F32) for s in (SHAPES[UP], *SHAPES[:2], *stat_pairs)],
        in_specs=[vmem_spec] * 13,
        out_specs=[any_spec] * 9,
        scratch_shapes=[pltpu.VMEM(SHAPES[UP], F32), dma],
        compiler_params=pltpu.CompilerParams(vmem_limit_bytes=VMEM_LIMIT),
        name="update",
    )(*held)
    up, down, gate, rd_n, cd_n, rg_n, cg_n, ru_n, cu_n = res
    flat = [v.reshape(-1) for v in (rg_n, cg_n, ru_n, cu_n, rd_n, cd_n)]
    return (gate, up, down, *flat)


def solution(mesh):
    act_spec = P(None, "row")
    cot_spec = P(None, "col")
    w_spec = P("row", "col")
    r_spec = P("row")
    c_spec = P("col")
    s_spec = P()
    return jax.shard_map(local_program, mesh=mesh, in_specs=(act_spec, act_spec, cot_spec, cot_spec, cot_spec, w_spec, w_spec, w_spec, r_spec, c_spec, r_spec, c_spec, r_spec, c_spec, s_spec, s_spec, s_spec), out_specs=(w_spec, w_spec, w_spec, r_spec, c_spec, r_spec, c_spec, r_spec, c_spec), check_vma=False)
```

```python
import jax
import jax.numpy as jnp
from jax import lax
from jax.experimental import pallas as pl
from jax.experimental.pallas import tpu as pltpu
from jax.sharding import PartitionSpec as P

EPS_SQ = 1e-30
EPS_SCALE = 1e-3
LANES = 128
K = 2048
ROWS, COLS = 4, 2
F32 = jnp.float32
BF16 = jnp.bfloat16
MESH = pl.DeviceIdType.MESH

DOWN, GATE, UP = 0, 1, 2
SHAPES = ((1408, 1024), (512, 2816), (512, 2816))
TOTALS = tuple((m * ROWS, n * COLS) for m, n in SHAPES)
PIECES = ((0, 256), (256, 512), (512, 1024), (1024, 1536), (1536, 2048))
GATE_BLOCKS = ((0, 1024), (1024, 2048), (2048, 2816))
UP_BLOCKS = ((0, 512), (512, 1536), (1536, 2048), (2048, 2816))
BLOCKS = tuple((GATE, *b) for b in GATE_BLOCKS) + tuple((UP, *b) for b in UP_BLOCKS)
EARLY_COLS = 16
CHUNK = 64
OTHERS = [(dc, dr) for dc in range(COLS) for dr in range(ROWS) if (dc, dr) != (0, 0)]


def interleave(dots, units):
    done = 0
    for i, dot in enumerate(dots):
        upto = len(units) * (i + 1) // len(dots)
        for unit in units[done:upto]:
            unit()
        done = upto
        dot()


def fold(x):
    return jnp.sum(x.reshape(x.shape[0] // 8, 8, x.shape[1]), axis=0)


def place():
    return lax.axis_index("data"), lax.axis_index("col"), lax.axis_index("row")


def peer(dc, dr):
    d, c, r = place()
    return (d, lax.rem(c + dc, COLS), lax.rem(r + dr, ROWS))


def signal_entry(barrier):
    for dc, dr in OTHERS:
        pl.semaphore_signal(barrier, inc=1, device_id=peer(dc, dr), device_id_type=MESH)


def remote(ref, send, recv, to):
    return pltpu.make_async_remote_copy(
        src_ref=ref, dst_ref=ref, send_sem=send, recv_sem=recv, device_id=to, device_id_type=MESH)


def scalar_tile(s, w, r):
    rows = [jnp.sum(v, axis=0, keepdims=True) for v in (s, w, r)]
    return jnp.concatenate(rows + [jnp.zeros((1, LANES), F32)], axis=0)


def step_of(mat, buf, rel, clip):
    mt, nt = TOTALS[mat]
    tot = buf[0]
    for i in range(1, ROWS * COLS):
        tot = tot + buf[i]
    tot = jnp.sum(tot, axis=1, keepdims=True)
    s, w, r = tot[0:1, :], tot[1:2, :], tot[2:3, :]
    r_mean = r * (1.0 / (COLS * mt))
    u_rms = jnp.sqrt(s * (1.0 / (mt * nt)) * r_mean)
    w_rms = jnp.sqrt(w * (1.0 / (mt * nt)))
    step = rel * jnp.maximum(EPS_SCALE, w_rms)
    k = step * jnp.sqrt(r_mean) / jnp.maximum(1.0, u_rms / clip)
    return jnp.broadcast_to(k, (8, LANES))


def main_kernel(
    x_hbm, h_hbm, dg_hbm, du_hbm, do_hbm, wg_hbm, wu_hbm, wd_hbm,
    rg_hbm, cg_hbm, ru_hbm, cu_hbm, rd_hbm, cd_hbm, beta, rel, clip,
    gu, wu, wd, wg, rd_new, cd_new, rg_new, cg_new, ru_new, cu_new, kap, abc_u, bv_u,
    gg, abc_g, bv_g,
    gd, ring, xt, hs, ht, rowacc, abc_d, cacc_d, cacc_g, cacc_u,
    bv_d, rd, cd, rg, cg, ru, cu, rbuf_d, rbuf_g, rbuf_u, cbuf_d, cbuf_g, cbuf_u, sbuf, sacc, wacc,
    sem, r_send, r_recv, c_send, c_recv, s_send, s_recv,
):
    G, W = (gd, gg, gu), (wd, wg, wu)
    d_hbm, w_hbm = (do_hbm, dg_hbm, du_hbm), (wd_hbm, wg_hbm, wu_hbm)
    r_old, c_old = (rd, rg, ru), (cd, cg, cu)
    r_new, c_new = (rd_new, rg_new, ru_new), (cd_new, cg_new, cu_new)
    abc, cacc, bv = (abc_d, abc_g, abc_u), (cacc_d, cacc_g, cacc_u), (bv_d, bv_g, bv_u)
    rbuf, cbuf = (rbuf_d, rbuf_g, rbuf_u), (cbuf_d, cbuf_g, cbuf_u)
    _, me_c, me_r = place()

    def piece_copies(p):
        ks = slice(*PIECES[p])
        return (
            pltpu.make_async_copy(h_hbm.at[ks, :], hs.at[ks, :], sem.at[2 * p]),
            pltpu.make_async_copy(do_hbm.at[ks, :512], ring.at[0, ks, :512], sem.at[2 * p + 1]),
        )

    x_copy = pltpu.make_async_copy(x_hbm, ring.at[2, :, :512], sem.at[10])
    right_copy = pltpu.make_async_copy(do_hbm.at[:, 512:], ring.at[0, :, 512:], sem.at[11])

    places = (
        ring.at[1], hs.at[:, :1024], ring.at[2, :, :768],
        ring.at[0, :, :512], ring.at[1], ring.at[0, :, 512:1024], hs.at[:, :768],
    )

    def d_copy(j):
        mat, n0, n1 = BLOCKS[j]
        return pltpu.make_async_copy(d_hbm[mat].at[:, n0:n1], places[j], sem.at[(12, 13, 6, 7, 10, 8, 12)[j]])

    old_copies = [
        pltpu.make_async_copy(src, dst, sem.at[i])
        for i, (src, dst) in enumerate(zip((rd_hbm, cd_hbm, rg_hbm, cg_hbm, ru_hbm, cu_hbm), (rd, cd, rg, cg, ru, cu)))
    ]

    def w_copy(mat):
        return pltpu.make_async_copy(w_hbm[mat], W[mat], sem.at[(9, 11, 13)[mat]])

    late = slice(EARLY_COLS, SHAPES[UP][1] // LANES)
    COL_GROUPS = ((DOWN, slice(0, 8), 0), (GATE, slice(0, 22), 0), (UP, late, 0), (UP, slice(0, EARLY_COLS), 1))
    EARLY = 3

    def start_row(mat):
        row_copy(mat).start()

    def row_copy(mat):
        return remote(rbuf[mat].at[me_c], r_send.at[0], r_recv.at[mat], peer(1, 0))

    def start_cols(group):
        mat, part, send = COL_GROUPS[group]
        for d in (1, 2, 3):
            remote(cbuf[mat].at[me_r, part], c_send.at[send], c_recv.at[group], peer(0, d)).start()

    def all_cols(group):
        mat, part, send = COL_GROUPS[group]
        return remote(cbuf[mat].at[0:3, part], c_send.at[send], c_recv.at[group], peer(0, 1))

    def start_tiles(mat):
        me = me_c * ROWS + me_r
        for dc, dr in OTHERS:
            remote(sbuf.at[mat, me], s_send.at[0], s_recv.at[mat], peer(dc, dr)).start()

    def all_tiles(mat):
        return remote(sbuf.at[mat, 0:7], s_send.at[0], s_recv.at[mat], peer(0, 1))

    def start(copies):
        for c in copies:
            c.start()

    def wait(copies):
        for c in copies:
            c.wait()

    def stats_units(mat, n0, n1):
        units = []
        for r in range(0, SHAPES[mat][0], CHUNK):
            def unit(r=r):
                part = None
                for t in range(n0 // LANES, n1 // LANES):
                    g = G[mat][r:r + CHUNK, t * LANES:(t + 1) * LANES]
                    q = g * g
                    part = q if part is None else part + q
                    col = fold(q)
                    cols = pl.ds(t * LANES, LANES)
                    cacc[mat][:, cols] = col if r == 0 else cacc[mat][:, cols] + col
                rows = pl.ds(r, CHUNK)
                rowacc[rows, :] = part if n0 == 0 else rowacc[rows, :] + part
            units.append(unit)
        return units

    def row_units(mat):
        units = []
        for i in range(SHAPES[mat][0] // LANES):
            def rows(i=i):
                block = rowacc[i * LANES:(i + 1) * LANES, :].T
                rbuf[mat][me_c, i:i + 1, :] = jnp.sum(block, axis=0, keepdims=True)
            units.append(rows)
        return units

    def col_units(mat, t0, t1):
        units = []
        for t in range(t0, t1):
            def cols(t=t):
                cbuf[mat][me_r, t:t + 1, :] = jnp.sum(
                    cacc[mat][:, t * LANES:(t + 1) * LANES], axis=0, keepdims=True)
            units.append(cols)
        return units

    def sums_units(mat):
        return row_units(mat) + col_units(mat, 0, SHAPES[mat][1] // LANES)

    def w2_units(mat):
        units = []
        m, n = SHAPES[mat]
        for i in range(m // CHUNK):
            def unit(i=i):
                acc = None
                for t in range(n // LANES):
                    w = W[mat][i * CHUNK:(i + 1) * CHUNK, t * LANES:(t + 1) * LANES]
                    f = fold(w * w)
                    acc = f if acc is None else acc + f
                wacc[mat, i] = acc
            units.append(unit)
        return units

    def factor_units(mat):
        m, n = SHAPES[mat]
        mt, nt = TOTALS[mat]

        def new():
            b2 = beta[0]
            rows = rbuf[mat][0] + rbuf[mat][1]
            cols = (cbuf[mat][0] + cbuf[mat][1]) + (cbuf[mat][2] + cbuf[mat][3])
            rn = b2 * r_old[mat][...] + (1.0 - b2) * (rows * (1.0 / nt) + EPS_SQ)
            cn = b2 * c_old[mat][...] + (1.0 - b2) * (cols * (1.0 / mt) + EPS_SQ)
            r_new[mat][...] = rn
            c_new[mat][...] = cn
            bv[mat][...] = lax.rsqrt(cn)

        units = [new]
        for i in range(m // LANES):
            def unit(i=i):
                a = lax.rsqrt(r_new[mat][i:i + 1, :])
                abc[mat][i * LANES:(i + 1) * LANES, :] = jnp.broadcast_to(a, (LANES, LANES)).T
            units.append(unit)
        return units

    def scale_units(mat):
        units = []
        m, n = SHAPES[mat]
        for i in range(m // CHUNK):
            def unit(i=i):
                acc = None
                rows = slice(i * CHUNK, (i + 1) * CHUNK)
                for t in range(n // LANES):
                    h = G[mat][rows, t * LANES:(t + 1) * LANES] * bv[mat][t:t + 1, :]
                    acc = h * h if acc is None else acc + h * h
                a = abc[mat][rows, :]
                sacc[mat, i] = fold(acc * (a * a))
            units.append(unit)
        return units

    def update_units(mat):
        def step():
            kap[mat] = step_of(mat, sbuf.at[mat], rel[0], clip[0])

        units = [step]
        m, n = SHAPES[mat]
        for r in range(0, m, CHUNK):
            def unit(r=r):
                ka = abc[mat][r:r + CHUNK, :] * kap[mat, 0:1, :]
                for t in range(n // LANES):
                    cols = slice(t * LANES, (t + 1) * LANES)
                    W[mat][r:r + CHUNK, cols] = (
                        W[mat][r:r + CHUNK, cols] - G[mat][r:r + CHUNK, cols] * ka * bv[mat][t:t + 1, :])
            units.append(unit)
        return units

    def tile_unit(mat):
        def unit():
            _, c, r = place()
            chunks = SHAPES[mat][0] // CHUNK
            sbuf[mat, c * ROWS + r] = scalar_tile(
                jnp.sum(sacc[mat, :chunks], axis=0), jnp.sum(wacc[mat, :chunks], axis=0), r_new[mat][...])
        return [unit]

    def h_units(p):
        k0, k1 = PIECES[p]
        units = []
        for k in range(k0, k1, 256):
            for i in range(0, SHAPES[DOWN][0], LANES):
                def unit(k=k, i=i):
                    ht[i:i + LANES, k:k + 256] = hs[k:k + 256, i:i + LANES].T
                units.append(unit)
        return units

    def x_units():
        units = []
        for k in range(0, K, 256):
            for i in range(0, 512, LANES):
                def unit(k=k, i=i):
                    xt[i:i + LANES, k:k + 256] = ring[2, k:k + 256, i:i + LANES].T
                units.append(unit)
        return units

    def down_dots(p):
        ks = slice(*PIECES[p])
        out = []
        for r in range(0, 1408, 352):
            def dot(r=r):
                rs = slice(r, r + 352)
                part = jnp.dot(ht[rs, ks], ring[0, ks, :512], preferred_element_type=F32)
                gd[rs, :512] = part if p == 0 else gd[rs, :512] + part
            out.append(dot)
        return out

    def right_dots():
        out = []
        for r in range(0, 1408, 352):
            def dot(r=r):
                rs = slice(r, r + 352)
                gd[rs, 512:] = jnp.dot(ht[rs, :], ring[0, :, 512:], preferred_element_type=F32)
            out.append(dot)
        return out

    def dots_of(j):
        mat, n0, n1 = BLOCKS[j]
        out = []

        def dot(r0, r1, c0, c1):
            def run():
                G[mat][r0:r1, n0 + c0:n0 + c1] = jnp.dot(
                    xt[r0:r1, :], places[j][:, c0:c1], preferred_element_type=F32)
            return run

        w = n1 - n0
        for c in range(0, w, 512):
            if c + 512 <= w:
                out.append(dot(0, 512, c, c + 512))
            else:
                out += [dot(0, 256, c, w), dot(256, 512, c, w)]
        return out

    def run(units):
        for unit in units:
            unit()

    for p in (0, 1, 2):
        start(piece_copies(p))
    barrier = pltpu.get_barrier_semaphore()
    signal_entry(barrier)
    wait(piece_copies(0))
    start(piece_copies(3))
    start(piece_copies(4))
    right_copy.start()
    x_copy.start()
    run(h_units(0))
    for p in range(4):
        wait(piece_copies(p + 1))
        if p == 1:
            d_copy(0).start()
        interleave(down_dots(p), h_units(p + 1))
    d_copy(1).start()
    interleave(down_dots(4), [])
    start(old_copies)
    right_copy.wait()
    x_copy.wait()
    interleave(right_dots(), x_units() + stats_units(DOWN, 0, 512))
    d_copy(2).start()
    d_copy(3).start()
    d_copy(5).start()
    w_copy(DOWN).start()

    d_copy(0).wait()
    wait(old_copies)
    interleave(dots_of(0), stats_units(DOWN, 512, 1024) + sums_units(DOWN))
    pl.semaphore_wait(barrier, len(OTHERS))
    start_row(DOWN)
    start_cols(DOWN)
    d_copy(4).start()
    w_copy(GATE).start()

    d_copy(1).wait()
    d_copy(2).wait()
    interleave(dots_of(1), stats_units(GATE, 0, 1024))
    interleave(dots_of(2), stats_units(GATE, 1024, 2048))
    d_copy(6).start()
    w_copy(UP).start()

    d_copy(3).wait()
    interleave(dots_of(3), stats_units(GATE, 2048, 2816) + sums_units(GATE))
    row_copy(DOWN).wait_send()
    all_cols(DOWN).wait_send()
    start_row(GATE)
    start_cols(GATE)

    d_copy(4).wait()
    d_copy(5).wait()
    row_copy(DOWN).wait_recv()
    all_cols(DOWN).wait_recv()
    interleave(dots_of(4) + dots_of(5), stats_units(UP, 0, 512) + factor_units(DOWN) + scale_units(DOWN))

    d_copy(6).wait()
    interleave(dots_of(6), stats_units(UP, 512, 1536) + stats_units(UP, 1536, 2048) + col_units(UP, 0, EARLY_COLS))
    start_cols(EARLY)

    run(stats_units(UP, 2048, 2816) + row_units(UP) + col_units(UP, EARLY_COLS, 22))
    row_copy(GATE).wait_send()
    all_cols(GATE).wait_send()
    start_row(UP)
    start_cols(UP)
    w_copy(DOWN).wait()
    w_copy(GATE).wait()
    w_copy(UP).wait()
    run(w2_units(DOWN) + tile_unit(DOWN))
    start_tiles(DOWN)
    row_copy(GATE).wait_recv()
    all_cols(GATE).wait_recv()
    run(factor_units(GATE) + scale_units(GATE) + w2_units(GATE) + tile_unit(GATE))
    all_tiles(DOWN).wait_send()
    start_tiles(GATE)
    run(w2_units(UP))
    all_cols(EARLY).wait_recv()
    row_copy(UP).wait_recv()
    all_cols(UP).wait_recv()
    run(factor_units(UP) + scale_units(UP) + tile_unit(UP))
    all_tiles(GATE).wait_send()
    start_tiles(UP)
    all_tiles(DOWN).wait_recv()
    run(update_units(DOWN))
    all_tiles(GATE).wait_recv()
    kap[GATE] = step_of(GATE, sbuf.at[GATE], rel[0], clip[0])
    row_copy(UP).wait_send()
    all_cols(UP).wait_send()
    all_cols(EARLY).wait_send()
    all_tiles(UP).wait_send()
    all_tiles(UP).wait_recv()
    kap[UP] = step_of(UP, sbuf.at[UP], rel[0], clip[0])


def update_kernel(
    gu, wu, wd, wg, rd, cd, rg, cg, ru, cu, kap, abc_u, bv_u, gg, abc_g, bv_g,
    wu_o, wd_o, wg_o, rd_o, cd_o, rg_o, cg_o, ru_o, cu_o, stage_g, stage_u, sem,
):
    copies = []

    def write(src, dst):
        copies.append(pltpu.make_async_copy(src, dst, sem))
        copies[-1].start()

    write(wd, wd_o)
    for src, dst in ((rd, rd_o), (cd, cd_o), (rg, rg_o), (cg, cg_o), (ru, ru_o), (cu, cu_o)):
        write(src, dst)
    for mat, g, w, abc, bv, stage, out in (
        (GATE, gg, wg, abc_g, bv_g, stage_g, wg_o), (UP, gu, wu, abc_u, bv_u, stage_u, wu_o),
    ):
        m, n = SHAPES[mat]
        k = kap[mat, 0:1, :]
        for r in range(0, m, CHUNK):
            rows = slice(r, r + CHUNK)
            ka = abc[rows, :] * k
            for t in range(n // LANES):
                cols = slice(t * LANES, (t + 1) * LANES)
                stage[rows, cols] = w[rows, cols] - g[rows, cols] * ka * bv[t:t + 1, :]
            write(stage.at[rows, :], out.at[rows, :])
    for copy in copies:
        copy.wait()


VMEM_LIMIT = 36900000


def local_program(x_in, h_act, d_gate, d_up, d_out, w_gate, w_up, w_down, r_gate, c_gate, r_up, c_up, r_down, c_down, beta_two, rel_step, clip_thr):
    any_spec = pl.BlockSpec(memory_space=pl.ANY)
    vmem_spec = pl.BlockSpec(memory_space=pltpu.VMEM)
    smem_spec = pl.BlockSpec(memory_space=pltpu.SMEM)

    def stat_shape(v):
        return (v // LANES, LANES)

    stats = [v.reshape(stat_shape(v.shape[0])) for v in (r_gate, c_gate, r_up, c_up, r_down, c_down)]
    beta, rel, clip = [v.reshape(1) for v in (beta_two, rel_step, clip_thr)]
    rows = [stat_shape(m) for m, n in SHAPES]
    cols = [stat_shape(n) for m, n in SHAPES]
    dma = pltpu.SemaphoreType.DMA

    stat_pairs = [s for pair in zip(rows, cols) for s in pair]
    outs = pl.pallas_call(
        main_kernel,
        out_shape=[pltpu.VMEM(SHAPES[UP], F32)] * 2 + [pltpu.VMEM(s, F32) for s in SHAPES[:2]]
        + [pltpu.VMEM(s, F32) for s in stat_pairs]
        + [pltpu.VMEM((3, 8, LANES), F32), pltpu.VMEM((512, LANES), F32), pltpu.VMEM(cols[UP], F32)]
        + [pltpu.VMEM(SHAPES[GATE], F32), pltpu.VMEM((512, LANES), F32), pltpu.VMEM(cols[GATE], F32)],
        in_specs=[any_spec] * 14 + [smem_spec] * 3,
        out_specs=[vmem_spec] * 16,
        scratch_shapes=[
            pltpu.VMEM(SHAPES[DOWN], F32),
            pltpu.VMEM((3, K, 1024), BF16),
            pltpu.VMEM((512, K), BF16),
            pltpu.VMEM((K, 1408), BF16),
            pltpu.VMEM((1408, K), BF16),
            pltpu.VMEM((1408, LANES), F32),
            pltpu.VMEM((1408, LANES), F32),
        ]
        + [pltpu.VMEM((8, n), F32) for m, n in SHAPES]
        + [pltpu.VMEM(cols[DOWN], F32)]
        + [pltpu.VMEM(s, F32) for s in stat_pairs]
        + [pltpu.VMEM((COLS, *s), F32) for s in rows]
        + [pltpu.VMEM((ROWS, *s), F32) for s in cols]
        + [
            pltpu.VMEM((3, ROWS * COLS, 4, LANES), F32),
            pltpu.VMEM((3, 22, 8, LANES), F32),
            pltpu.VMEM((3, 22, 8, LANES), F32),
            dma((14,)), dma((1,)), dma((3,)), dma((2,)), dma((4,)), dma((1,)), dma((3,)),
        ],
        compiler_params=pltpu.CompilerParams(
            collective_id=0, has_side_effects=True, vmem_limit_bytes=VMEM_LIMIT),
        name="main",
    )(
        *[pltpu.with_memory_space_constraint(v, pltpu.HBM)
          for v in (x_in, h_act, d_gate, d_up, d_out, w_gate, w_up, w_down, *stats)],
        beta, rel, clip)
    held = [pltpu.with_memory_space_constraint(v, pltpu.VMEM) for v in outs]
    res = pl.pallas_call(
        update_kernel,
        out_shape=[jax.ShapeDtypeStruct(s, F32) for s in (SHAPES[UP], *SHAPES[:2], *stat_pairs)],
        in_specs=[vmem_spec] * 16,
        out_specs=[any_spec] * 9,
        scratch_shapes=[pltpu.VMEM(SHAPES[GATE], F32), pltpu.VMEM(SHAPES[UP], F32), dma],
        compiler_params=pltpu.CompilerParams(vmem_limit_bytes=VMEM_LIMIT),
        name="update",
    )(*held)
    up, down, gate, rd_n, cd_n, rg_n, cg_n, ru_n, cu_n = res
    flat = [v.reshape(-1) for v in (rg_n, cg_n, ru_n, cu_n, rd_n, cd_n)]
    return (gate, up, down, *flat)


def solution(mesh):
    act_spec = P(None, "row")
    cot_spec = P(None, "col")
    w_spec = P("row", "col")
    r_spec = P("row")
    c_spec = P("col")
    s_spec = P()
    return jax.shard_map(local_program, mesh=mesh, in_specs=(act_spec, act_spec, cot_spec, cot_spec, cot_spec, w_spec, w_spec, w_spec, r_spec, c_spec, r_spec, c_spec, r_spec, c_spec, s_spec, s_spec, s_spec), out_specs=(w_spec, w_spec, w_spec, r_spec, c_spec, r_spec, c_spec, r_spec, c_spec), check_vma=False)
```
